32 devices in a mesh: owner: 4 (over y, x), rows: 8 (over z, core).
Axes of the slice: x: 2, y: 2, z: 4, core: 2. Of those that a mesh axis runs over, the one named last changes fastest.
Arguments:
- w_gate: float32 [64, 2048, 1024], P('owner', 'rows'), may hold values from -0.1875 to 0.1875
- avg_gate: bfloat16 [64, 2048, 1024], P('owner', 'rows'), may hold values from -0.0625 to 0.0625
- w_up: float32 [64, 2048, 1024], P('owner', 'rows'), may hold values from -0.1875 to 0.1875
- avg_up: bfloat16 [64, 2048, 1024], P('owner', 'rows'), may hold values from -0.0625 to 0.0625
- w_down: float32 [64, 1024, 2048], P('owner', None, 'rows'), may hold values from -0.25 to 0.25
- avg_down: bfloat16 [64, 1024, 2048], P('owner', None, 'rows'), may hold values from -0.09375 to 0.09375
- router_weight: float32 [2048, 64], P('rows', 'owner'), may hold values from -0.125 to 0.125
- router_gain: float32 [2048], P('rows'), may hold values from 0.25 to 1.75
Outputs:
- serve_gate: bfloat16 [64, 2048, 1024], P('owner', None, 'rows')
- serve_up: bfloat16 [64, 2048, 1024], P('owner', None, 'rows')
- serve_down: bfloat16 [64, 1024, 2048], P('owner', 'rows')
- scale_gate: float32 [64, 1024], P('owner', 'rows')
- scale_up: float32 [64, 1024], P('owner', 'rows')
- scale_down: float32 [64, 1024], P('owner', 'rows')
- serve_router: bfloat16 [2048, 64], replicated
The draws below stay inside these ranges and needn't reach their ends.
All inputs are finite; a program needn't handle non-finite values.
Results may differ from the reference program's by a relative error of at most 0.0015.
Values may be sent and summed in bfloat16 or wider, within the bound.
A program may use at most 192 MiB of HBM per device.

```python
import jax
import jax.numpy as jnp
from jax import lax

EXPERTS = 64
D_MODEL = 2048
D_EXPERT = 1024


def raised(drawn, stream_key, source, target, shards_of, factor):
    owner, partner = [(jnp.arange(drawn.shape[position]) // (drawn.shape[position] // shards_of)).reshape([-1 if axis == position else 1 for axis in range(drawn.ndim)]) for position in (source, target)]
    chosen = jax.random.permutation(stream_key, shards_of)[partner]
    strong = (owner == chosen) | (owner == (partner + shards_of // 2) % shards_of)
    return jnp.where(strong, factor * drawn, drawn)


def shard_levels(key, dims, shards, smallest, top_value):
    factor_of = 1.0
    for position, blocks in shards:
        draws = jax.random.uniform(jax.random.fold_in(jax.random.fold_in(key, 6), position), (blocks,), jnp.float32, smallest / len(shards), top_value / len(shards))
        factor_of = factor_of * jnp.repeat(jnp.exp(draws), dims[position] // blocks).reshape((-1,) + (1,) * (len(dims) - 1 - position))
    return factor_of


def centred(own_key, dims, spread, limit, pieces=(), held_as=jnp.bfloat16):
    factor_of = shard_levels(own_key, dims, pieces, -0.22, 0.18) if pieces else 1.0
    entries = jax.random.normal(own_key, dims, jnp.float32) * spread * factor_of
    return jnp.minimum(jnp.maximum(entries, -limit), limit).astype(held_as)


def noise_with(stream_key, shape, deviation, limit, cuts, heavy, dtype=jnp.bfloat16):
    result = deviation * jax.random.normal(stream_key, shape, jnp.float32)
    if cuts:
        result = result * shard_levels(stream_key, shape, cuts, -0.22, 0.18)
    return jnp.clip(raised(result, jax.random.fold_in(stream_key, 3), *heavy), -limit, limit).astype(dtype)


def setup_inputs(seed: int = 0) -> dict:
    streams_of = jax.random.split(jax.random.key(seed), 9)
    w_gate = noise_with(streams_of[0], (EXPERTS, D_MODEL, D_EXPERT), D_MODEL ** -0.5, 0.1875, ((0, 4), (1, 8)), (1, 2, 8, 2.0), jnp.float32)
    avg_gate = centred(streams_of[1], (EXPERTS, D_MODEL, D_EXPERT), (D_MODEL * 4) ** -0.5, 0.0625, ((0, 4), (1, 8)))
    w_up = noise_with(streams_of[2], (EXPERTS, D_MODEL, D_EXPERT), D_MODEL ** -0.5, 0.1875, ((0, 4), (1, 8)), (1, 2, 8, 2.0), jnp.float32)
    avg_up = centred(streams_of[3], (EXPERTS, D_MODEL, D_EXPERT), (D_MODEL * 4) ** -0.5, 0.0625, ((0, 4), (1, 8)))
    w_down = noise_with(streams_of[4], (EXPERTS, D_EXPERT, D_MODEL), D_EXPERT ** -0.5, 0.25, ((0, 4), (2, 8)), (2, 1, 8, 2.0), jnp.float32)
    avg_down = centred(streams_of[5], (EXPERTS, D_EXPERT, D_MODEL), (D_EXPERT * 4) ** -0.5, 0.09375, ((0, 4), (2, 8)))
    router_weight = centred(streams_of[6], (D_MODEL, EXPERTS), D_MODEL ** -0.5, 0.125, ((0, 8), (1, 4)), jnp.float32)
    router_gain = jnp.clip(1.0 + 0.15 * jax.random.normal(streams_of[7], (D_MODEL,), jnp.float32), 0.25, 1.75)
    return {"w_gate": w_gate, "avg_gate": avg_gate, "w_up": w_up, "avg_up": avg_up, "w_down": w_down, "avg_down": avg_down, "router_weight": router_weight, "router_gain": router_gain}


def reference(w_gate, avg_gate, w_up, avg_up, w_down, avg_down, router_weight, router_gain):
    fresh_gate = w_gate + avg_gate.astype(jnp.float32)
    fresh_up = w_up + avg_up.astype(jnp.float32)
    fresh_down = w_down + avg_down.astype(jnp.float32)
    scale_gate = jnp.sqrt(lax.optimization_barrier(jnp.sum(fresh_gate * fresh_gate, axis=1)))
    serve_gate = (fresh_gate / jnp.expand_dims(scale_gate, 1)).astype(jnp.bfloat16)
    scale_up = jnp.sqrt(lax.optimization_barrier(jnp.sum(fresh_up * fresh_up, axis=1)))
    serve_up = (fresh_up / jnp.expand_dims(scale_up, 1)).astype(jnp.bfloat16)
    scale_down = jnp.sqrt(lax.optimization_barrier(jnp.sum(fresh_down * fresh_down, axis=2)))
    serve_down = (fresh_down / jnp.expand_dims(scale_down, 2)).astype(jnp.bfloat16)
    serve_router = (router_weight * router_gain[:, None]).astype(jnp.bfloat16)
    return (serve_gate, serve_up, serve_down, scale_gate, scale_up, scale_down, serve_router)
```

```python
import functools

import jax
import jax.numpy as jnp
from jax import lax
from jax.experimental import pallas as pl
from jax.experimental.pallas import tpu as pltpu
from jax.sharding import PartitionSpec as P

LANES = 128
HEAD = 3
NEXT = 3
RING = 4
TAIL = 2
MESH = pl.DeviceIdType.MESH


def remote(src, dst, send, recv, peer, axis="rows"):
    return pltpu.make_async_remote_copy(
        src_ref=src, dst_ref=dst, send_sem=send, recv_sem=recv, device_id={axis: peer}, device_id_type=MESH
    )


def regroup(
    parts, owners,
    wg, ag, wu, au, wd, ad, rw, gain,
    og, ou, od, ot, oscale, orouter,
    wbuf, abuf, wdbuf, adbuf, sg, su, sd, part, heard, factors, scales, rwbuf, gainbuf, piece, router,
    in_sem, down_sem, sum_send, sum_recv, factor_send, factor_recv, data_send, data_recv, kept, piece_send, piece_recv,
    router_send, router_recv, small,
):
    me = lax.axis_index("rows")
    own = lax.axis_index("owner")
    experts, high = wg.shape[0], wg.shape[1]
    tall, deep = wd.shape[1:]
    units = 3 * experts
    tail = ot.shape[1]

    def peer(k):
        return lax.rem(me + k, parts)

    def fetch(w, a, e, wv, av, sem, slot):
        pltpu.make_async_copy(w.at[e], wv.at[slot], sem.at[0, slot]).start()
        pltpu.make_async_copy(a.at[e], av.at[slot], sem.at[1, slot]).start()

    def fetched(w, a, e, wv, av, sem, slot):
        pltpu.make_async_copy(w.at[e], wv.at[slot], sem.at[0, slot]).wait()
        pltpu.make_async_copy(a.at[e], av.at[slot], sem.at[1, slot]).wait()

    def stream(w, a, wv, av, sem, base, first, count, body):
        for i in range(min(RING - 1, count)):
            fetch(w, a, first + i, wv, av, sem, base + i)

        @pl.loop(0, count)
        def _(i):
            slot = base + lax.rem(i, RING)
            fetched(w, a, first + i, wv, av, sem, slot)

            @pl.when(i + RING - 1 < count)
            def _():
                fetch(w, a, first + i + RING - 1, wv, av, sem, base + lax.rem(i + RING - 1, RING))

            body(first + i, slot)

    def lanes(p):
        return pl.ds(pl.multiple_of(p * LANES, LANES), LANES)

    def columns_sum(unit, slot):
        @pl.loop(0, parts)
        def _(p):
            fresh = wbuf[slot, :, lanes(p)] + abuf[slot, :, lanes(p)].astype(jnp.float32)
            part[p, unit] = jnp.sum(fresh * fresh, axis=0, keepdims=True)

    def rows_sum(unit, slot):
        @pl.loop(0, parts)
        def _(p):
            fresh = wdbuf[slot, lanes(p), :] + adbuf[slot, lanes(p), :].astype(jnp.float32)
            square = fresh * fresh
            folded = square[:, :LANES]
            for start in range(LANES, deep, LANES):
                folded = folded + square[:, start : start + LANES]
            part[p, unit] = jnp.sum(folded.T, axis=0, keepdims=True)

    def columns_norm(unit, e, slot, send):
        @pl.loop(0, parts)
        def _(p):
            fresh = wbuf[slot, :, lanes(p)] + abuf[slot, :, lanes(p)].astype(jnp.float32)
            send[e, p] = (fresh * factors[p, unit]).astype(send.dtype)

    def rows_norm(unit, e, slot):
        @pl.loop(0, parts)
        def _(p):
            factor = jnp.broadcast_to(factors[p, unit], (LANES, LANES)).T
            for start in range(0, deep, LANES):
                fresh = wdbuf[slot, lanes(p), start : start + LANES]
                fresh = fresh + adbuf[slot, lanes(p), start : start + LANES].astype(jnp.float32)
                sd[e, p, :, start : start + LANES] = (fresh * factor).astype(sd.dtype)

    def send_sums(group, first, count):
        @pl.loop(1, parts)
        def _(k):
            remote(
                part.at[peer(k), pl.ds(first, count)], heard.at[me, pl.ds(first, count)],
                sum_send.at[group], sum_recv.at[group], peer(k),
            ).start()

    def send_factors(group, first, count):
        whole = heard.at[pl.ds(0, parts - 1), pl.ds(first, count)]
        pltpu.make_async_copy(whole, whole, sum_recv.at[group]).wait()

        @pl.loop(first, first + count)
        def _(unit):
            total = part[me, unit]
            for k in range(1, parts):
                total = total + heard[peer(k), unit]
            scale = jnp.sqrt(total)
            scales[unit] = scale
            factors[me, unit] = 1.0 / scale

        @pl.loop(1, parts)
        def _(k):
            mine = factors.at[me, pl.ds(first, count)]
            remote(mine, mine, factor_send.at[group], factor_recv.at[group], peer(k)).start()

    def take_factors(group, first, count):
        whole = factors.at[pl.ds(0, parts - 1), pl.ds(first, count)]
        pltpu.make_async_copy(whole, whole, factor_recv.at[group]).wait()

    def push(kind, e):
        send, stage = ((sg, og), (su, ou), (sd, od))[kind]
        if kind < 2:
            place = stage.at[e, pl.ds(pl.multiple_of(me * high, high), high), :]
        else:
            place = stage.at[e, :, pl.ds(pl.multiple_of(me * deep, deep), deep)]

        @pl.loop(1, parts)
        def _(k):
            remote(send.at[e, peer(k)], place, data_send.at[kind], data_recv.at[kind], peer(k)).start()

        pltpu.make_async_copy(send.at[e, me], place, kept.at[kind]).start()

    barrier = pltpu.get_barrier_semaphore()
    early = HEAD + NEXT
    for i in range(early):
        fetch(wg, ag, i, wbuf, abuf, in_sem, i)
    pltpu.make_async_copy(rw, rwbuf, small.at[0]).start()
    pltpu.make_async_copy(gain, gainbuf, small.at[1]).start()

    @pl.loop(1, parts)
    def _(k):
        pl.semaphore_signal(barrier, inc=1, device_id={"rows": peer(k)}, device_id_type=MESH)

    for k in range(1, owners):
        pl.semaphore_signal(barrier, inc=1, device_id={"owner": lax.rem(own + k, owners)}, device_id_type=MESH)

    @pl.loop(0, HEAD)
    def _(i):
        fetched(wg, ag, i, wbuf, abuf, in_sem, i)
        columns_sum(i, i)

    pl.semaphore_wait(barrier, parts - 1 + owners - 1)
    send_sums(0, 0, HEAD)

    pltpu.make_async_copy(rw, rwbuf, small.at[0]).wait()
    pltpu.make_async_copy(gain, gainbuf, small.at[1]).wait()
    piece[...] = (rwbuf[...] * gainbuf[...]).astype(piece.dtype)

    @pl.loop(HEAD, early)
    def _(i):
        fetched(wg, ag, i, wbuf, abuf, in_sem, i)
        columns_sum(i, i)

    strip = router.at[own, :, pl.ds(pl.multiple_of(me * high, high), high)]
    send_factors(0, 0, HEAD)
    send_sums(1, HEAD, NEXT)
    take_factors(0, 0, HEAD)

    columns_norm(0, 0, 0, sg)
    columns_norm(1, 1, 1, sg)
    push(0, 0)
    send_factors(1, HEAD, NEXT)
    columns_norm(2, 2, 2, sg)
    push(0, 1)

    @pl.loop(1, parts)
    def _(k):
        remote(piece, strip, piece_send, piece_recv, peer(k)).start()

    router[own, :, pl.ds(pl.multiple_of(me * high, high), high)] = piece[...]
    push(0, 2)

    stream(wg, ag, wbuf, abuf, in_sem, early, early, experts - early, columns_sum)
    stream(wu, au, wbuf, abuf, in_sem, early, 0, experts, lambda e, slot: columns_sum(experts + e, slot))
    stream(wd, ad, wdbuf, adbuf, down_sem, 0, 0, experts, lambda e, slot: rows_sum(2 * experts + e, slot))

    send_sums(2, early, units - early)
    take_factors(1, HEAD, NEXT)

    @pl.loop(HEAD, early)
    def _(i):
        columns_norm(i, i, i, sg)

    push(0, HEAD)
    send_factors(2, early, units - early)

    @pl.loop(HEAD + 1, early)
    def _(i):
        push(0, i)

    gathered = router.at[own, :, pl.ds(0, (parts - 1) * high)]
    pltpu.make_async_copy(gathered, gathered, piece_recv).wait()
    for k in range(1, owners):
        remote(
            router.at[own], router.at[own], router_send, router_recv, lax.rem(own + k, owners), "owner"
        ).start()

    pltpu.make_async_copy(scales, oscale, small.at[0]).start()
    take_factors(2, early, units - early)

    def gate(e, slot):
        columns_norm(e, e, slot, sg)

        @pl.when(e > early)
        def _():
            push(0, e - 1)

    def up(e, slot):
        columns_norm(experts + e, e, slot, su)

        @pl.when(e > 0)
        def _():
            push(1, e - 1)

    def down(e, slot):
        rows_norm(2 * experts + e, e, slot)

        @pl.when((e > 0) & (e <= experts - tail))
        def _():
            push(2, e - 1)

    stream(wg, ag, wbuf, abuf, in_sem, early, early, experts - early, gate)
    push(0, experts - 1)
    stream(wu, au, wbuf, abuf, in_sem, early, 0, experts, up)
    push(1, experts - 1)
    stream(wd, ad, wdbuf, adbuf, down_sem, 0, 0, experts, down)

    for i in range(tail):
        pltpu.make_async_copy(sd.at[experts - tail + i], ot.at[:, i], kept.at[3]).start()

    arrived = router.at[pl.ds(0, owners - 1)]
    pltpu.make_async_copy(arrived, arrived, router_recv).wait()
    pltpu.make_async_copy(router, orouter, small.at[1]).start()

    for group, first, count in ((0, 0, HEAD), (1, HEAD, NEXT), (2, early, units - early)):
        whole = part.at[pl.ds(0, parts - 1), pl.ds(first, count)]
        pltpu.make_async_copy(whole, whole, sum_send.at[group]).wait()
        pltpu.make_async_copy(whole, whole, factor_send.at[group]).wait()
    pltpu.make_async_copy(gathered, gathered, piece_send).wait()
    pltpu.make_async_copy(arrived, arrived, router_send).wait()
    pltpu.make_async_copy(scales, oscale, small.at[0]).wait()
    pltpu.make_async_copy(router, orouter, small.at[1]).wait()
    pltpu.make_async_copy(sd.at[pl.ds(experts - tail, tail)], sd.at[pl.ds(experts - tail, tail)], kept.at[3]).wait()
    for kind, (send, stage) in enumerate(((sg, og), (su, ou), (sd, od))):
        count = experts - tail if kind == 2 else experts
        pltpu.make_async_copy(send.at[pl.ds(0, count), 0], send.at[pl.ds(0, count), 0], kept.at[kind]).wait()
        most = send.at[pl.ds(0, count), pl.ds(0, parts - 1)]
        pltpu.make_async_copy(most, most, data_send.at[kind]).wait()
        pltpu.make_async_copy(most, most, data_recv.at[kind]).wait()


def copied(x, *refs):
    refs[-1][...] = x[...]


def stack_columns(x, *refs):
    o = refs[-1]
    deep = x.shape[3]
    for source in range(x.shape[0]):
        o[:, :, source * deep : (source + 1) * deep] = x[source]


def placed(body, count, step, x, x_spec, out_shape, first=0, held=None):
    inputs, specs, aliases = [x], [x_spec], {}
    if held is not None:
        inputs, specs, aliases = [x, held], [x_spec, pl.BlockSpec(memory_space=pl.ANY)], {1: 0}
    moved = int(count * 2**21)
    return pl.pallas_call(
        body,
        grid=(count // step,),
        in_specs=specs,
        out_specs=pl.BlockSpec((step,) + out_shape[1:], lambda e: (e + first // step, 0, 0)),
        out_shape=jax.ShapeDtypeStruct(out_shape, jnp.bfloat16),
        input_output_aliases=aliases,
        cost_estimate=pl.CostEstimate(flops=moved, bytes_accessed=moved, transcendentals=0),
        compiler_params=pltpu.CompilerParams(
            dimension_semantics=("arbitrary",), vmem_limit_bytes=50 * 2**20
        ),
    )(*inputs)


def whole_experts(shape, step):
    return pl.BlockSpec((step,) + shape[1:], lambda e: (e, 0, 0))


def shards(parts, owners, w_gate, avg_gate, w_up, avg_up, w_down, avg_down, router_weight, router_gain):
    experts, high, wide = w_gate.shape
    tall, deep = w_down.shape[1:]
    block, slab = wide // parts, tall // parts
    units, slots = 3 * experts, HEAD + NEXT + RING
    columns = router_weight.shape[1]
    f32, bf16 = jnp.float32, jnp.bfloat16
    any_spec = pl.BlockSpec(memory_space=pl.ANY)
    shape_columns, shape_down = (experts, high * parts, block), (experts, slab, deep * parts)
    dma = pltpu.SemaphoreType.DMA

    stage_gate, stage_up, stage_down, last, scales, routers = pl.pallas_call(
        functools.partial(regroup, parts, owners),
        in_specs=[any_spec] * 8,
        out_specs=[any_spec] * 6,
        out_shape=[
            jax.ShapeDtypeStruct(shape_columns, bf16),
            jax.ShapeDtypeStruct(shape_columns, bf16),
            jax.ShapeDtypeStruct(shape_down, bf16),
            jax.ShapeDtypeStruct((parts, TAIL, slab, deep), bf16),
            jax.ShapeDtypeStruct((units, 1, LANES), f32),
            jax.ShapeDtypeStruct((owners, columns, parts * high), bf16),
        ],
        scratch_shapes=[
            pltpu.VMEM((slots, high, wide), f32),
            pltpu.VMEM((slots, high, wide), bf16),
            pltpu.VMEM((RING, tall, deep), f32),
            pltpu.VMEM((RING, tall, deep), bf16),
            pltpu.VMEM((experts, parts, high, block), bf16),
            pltpu.VMEM((experts, parts, high, block), bf16),
            pltpu.VMEM((experts, parts, slab, deep), bf16),
            pltpu.VMEM((parts, units, 1, LANES), f32),
            pltpu.VMEM((parts, units, 1, LANES), f32),
            pltpu.VMEM((parts, units, 1, LANES), f32),
            pltpu.VMEM((units, 1, LANES), f32),
            pltpu.VMEM((columns, high), f32),
            pltpu.VMEM((1, high), f32),
            pltpu.VMEM((columns, high), bf16),
            pltpu.VMEM((owners, columns, parts * high), bf16),
            dma((2, slots)), dma((2, RING)),
            dma((3,)), dma((3,)), dma((3,)), dma((3,)),
            dma((3,)), dma((3,)), dma((4,)),
            dma, dma, dma, dma, dma((2,)),
        ],
        cost_estimate=pl.CostEstimate(flops=2**30, bytes_accessed=2**28, transcendentals=0),
        compiler_params=pltpu.CompilerParams(
            collective_id=0, has_side_effects=True, vmem_limit_bytes=60 * 2**20
        ),
    )(w_gate, avg_gate, w_up, avg_up, w_down, avg_down, router_weight.T, router_gain.reshape(1, high))

    got = lax.all_to_all(last, "rows", split_axis=0, concat_axis=0, tiled=True)
    step = 2
    serve_gate = placed(copied, experts, step, stage_gate, whole_experts(shape_columns, step), shape_columns)
    serve_up = placed(copied, experts, step, stage_up, whole_experts(shape_columns, step), shape_columns)
    serve_down = placed(copied, experts - TAIL, step, stage_down, whole_experts(shape_down, step), shape_down)
    serve_router = routers.reshape(owners * columns, parts * high).T
    scales = scales.reshape(3, experts, LANES)
    serve_down = placed(
        stack_columns, TAIL, TAIL, got, pl.BlockSpec(got.shape, lambda e: (0, 0, 0, 0)), shape_down,
        experts - TAIL, serve_down,
    )
    return (serve_gate, serve_up, serve_down, scales[0], scales[1], scales[2], serve_router)


def plain_shards(w_gate, avg_gate, w_up, avg_up, w_down, avg_down, router_weight, router_gain):
    def served(w, a, axis, split):
        fresh = w + a.astype(jnp.float32)
        scale = jnp.sqrt(lax.psum(jnp.sum(fresh * fresh, axis=axis), "rows"))
        narrow = (fresh / jnp.expand_dims(scale, axis)).astype(jnp.bfloat16)
        serve = lax.all_to_all(narrow, "rows", split_axis=split, concat_axis=axis, tiled=True)
        width = serve.shape[split]
        return serve, lax.dynamic_slice_in_dim(scale, lax.axis_index("rows") * width, width, axis=1)

    serve_gate, scale_gate = served(w_gate, avg_gate, 1, 2)
    serve_up, scale_up = served(w_up, avg_up, 1, 2)
    serve_down, scale_down = served(w_down, avg_down, 2, 1)
    part_router = (router_weight * router_gain[:, None]).astype(jnp.bfloat16)
    row_router = lax.all_gather(part_router, "rows", axis=0, tiled=True)
    serve_router = lax.all_gather(row_router, "owner", axis=1, tiled=True)
    return (serve_gate, serve_up, serve_down, scale_gate, scale_up, scale_down, serve_router)


def solution(mesh):
    parts, owners = mesh.shape["rows"], mesh.shape["owner"]

    def dispatched(*args):
        experts, high, wide = args[0].shape
        tall, deep = args[4].shape[1:]
        block, slab = wide // parts, tall // parts
        columns = args[6].shape[1]
        aligned = block == LANES and slab == LANES and deep % LANES == 0 and high % LANES == 0
        aligned = aligned and high <= 256 and deep <= 256 and experts <= 16 and experts % 2 == 0
        aligned = aligned and experts > HEAD + NEXT and columns % 16 == 0 and parts > 1 and owners > 1
        return shards(parts, owners, *args) if aligned else plain_shards(*args)

    return jax.shard_map(
        dispatched,
        mesh=mesh,
        in_specs=(
            P("owner", "rows", None),
            P("owner", "rows", None),
            P("owner", "rows", None),
            P("owner", "rows", None),
            P("owner", None, "rows"),
            P("owner", None, "rows"),
            P("rows", "owner"),
            P("rows"),
        ),
        out_specs=(
            P("owner", None, "rows"),
            P("owner", None, "rows"),
            P("owner", "rows", None),
            P("owner", "rows"),
            P("owner", "rows"),
            P("owner", "rows"),
            P(),
        ),
        check_vma=False,
    )
```

```python
import functools

import jax
import jax.numpy as jnp
from jax import lax
from jax.experimental import pallas as pl
from jax.experimental.pallas import tpu as pltpu
from jax.sharding import PartitionSpec as P

LANES = 128
HEAD = 2
EARLY = 8
RING = 4
TAIL = 2
MESH = pl.DeviceIdType.MESH


def remote(src, dst, send, recv, peer, axis="rows"):
    return pltpu.make_async_remote_copy(
        src_ref=src, dst_ref=dst, send_sem=send, recv_sem=recv, device_id={axis: peer}, device_id_type=MESH
    )


def regroup(
    parts, owners,
    wg, ag, wu, au, wd, ad, rw, gain,
    og, ou, od, ot, oscale, orouter,
    wbuf, abuf, wdbuf, adbuf, sg, su, sd, direct, near, early, early_heard, early_factors,
    rest, rest_heard, factors, scales, rwbuf, gainbuf, piece, router,
    in_sem, down_sem, direct_send, direct_recv, early_send, early_recv, give_send, give_recv, back_send, back_recv,
    data_send, data_recv, kept, piece_send, piece_recv, router_send, router_recv, small,
):
    me = lax.axis_index("rows")
    own = lax.axis_index("owner")
    experts, high = wg.shape[0], wg.shape[1]
    deep = wd.shape[2]
    tail = ot.shape[1]
    levels = parts.bit_length() - 1
    bits = [lax.rem(me // 2**level, 2) for level in range(levels)]

    def peer(k):
        return lax.rem(me + k, parts)

    def mirrored(index):
        return sum(lax.rem(index // 2**i, 2) * 2 ** (levels - 1 - i) for i in range(levels))

    def fetch(w, a, e, wv, av, sem, slot):
        pltpu.make_async_copy(w.at[e], wv.at[slot], sem.at[0, slot]).start()
        pltpu.make_async_copy(a.at[e], av.at[slot], sem.at[1, slot]).start()

    def fetched(w, a, e, wv, av, sem, slot):
        pltpu.make_async_copy(w.at[e], wv.at[slot], sem.at[0, slot]).wait()
        pltpu.make_async_copy(a.at[e], av.at[slot], sem.at[1, slot]).wait()

    def landed(ref, sem):
        pltpu.make_async_copy(ref, ref, sem).wait()

    def stream(w, a, wv, av, sem, base, first, count, body):
        for i in range(min(RING - 1, count)):
            fetch(w, a, first + i, wv, av, sem, base + i)

        @pl.loop(0, count)
        def _(i):
            slot = base + lax.rem(i, RING)
            fetched(w, a, first + i, wv, av, sem, slot)

            @pl.when(i + RING - 1 < count)
            def _():
                fetch(w, a, first + i + RING - 1, wv, av, sem, base + lax.rem(i + RING - 1, RING))

            body(first + i, slot)

    def lanes(p):
        return pl.ds(pl.multiple_of(p * LANES, LANES), LANES)

    def columns_sum(slot, put):
        @pl.loop(0, parts)
        def _(s):
            p = mirrored(s)
            fresh = wbuf[slot, :, lanes(p)] + abuf[slot, :, lanes(p)].astype(jnp.float32)
            put(s, jnp.sum(fresh * fresh, axis=0, keepdims=True))

    def rows_sum(slot, put):
        @pl.loop(0, parts)
        def _(s):
            p = mirrored(s)
            fresh = wdbuf[slot, lanes(p), :] + adbuf[slot, lanes(p), :].astype(jnp.float32)
            square = fresh * fresh
            folded = square[:, :LANES]
            for start in range(LANES, deep, LANES):
                folded = folded + square[:, start : start + LANES]
            put(s, jnp.sum(folded.T, axis=0, keepdims=True))

    def columns_norm(take, e, slot, send):
        @pl.loop(0, parts)
        def _(s):
            p = mirrored(s)
            fresh = wbuf[slot, :, lanes(p)] + abuf[slot, :, lanes(p)].astype(jnp.float32)
            send[e, p] = (fresh * take(s)).astype(send.dtype)

    def rows_norm(take, e, slot):
        @pl.loop(0, parts)
        def _(s):
            p = mirrored(s)
            factor = jnp.broadcast_to(take(s), (LANES, LANES)).T
            for start in range(0, deep, LANES):
                fresh = wdbuf[slot, lanes(p), start : start + LANES]
                fresh = fresh + adbuf[slot, lanes(p), start : start + LANES].astype(jnp.float32)
                sd[e, p, :, start : start + LANES] = (fresh * factor).astype(sd.dtype)

    def put_head(unit):
        def put(s, row):
            direct[me, unit, pl.ds(s, 1), :] = row
            early[s, pl.ds(unit, 1), :] = row

        return put

    def put_in(ref, row):
        def put(s, value):
            ref[s, pl.ds(row, 1), :] = value

        return put

    def taken(ref, row):
        return lambda s: ref[s, pl.ds(row, 1), :]

    def push(kind, e):
        send, stage = ((sg, og), (su, ou), (sd, od))[kind]
        if kind < 2:
            place = stage.at[e, pl.ds(pl.multiple_of(me * high, high), high), :]
        else:
            place = stage.at[e, :, pl.ds(pl.multiple_of(me * deep, deep), deep)]

        @pl.loop(1, parts)
        def _(k):
            remote(send.at[e, peer(k)], place, data_send.at[kind], data_recv.at[kind], peer(k)).start()

        pltpu.make_async_copy(send.at[e, me], place, kept.at[kind]).start()

    def span(level):
        half = parts >> (level + 1)
        start = sum(bits[i] * (parts >> (i + 1)) for i in range(level))
        return start + bits[level] * half, start + (1 - bits[level]) * half, half, me + (1 - 2 * bits[level]) * 2**level

    def heard(level):
        return rest_heard.at[pl.ds(parts - (parts >> level), parts >> (level + 1))]

    def give(level):
        _, away, half, partner = span(level)
        remote(rest.at[pl.ds(away, half)], heard(level), give_send.at[level], give_recv.at[level], partner).start()

    def gain_level(level):
        keep, _, half, _ = span(level)
        landed(heard(level), give_recv.at[level])
        first = parts - (parts >> level)
        for i in range(half):
            rest[keep + i] = rest[keep + i] + rest_heard[first + i]

    def back(level):
        keep, _, half, partner = span(level)
        mine = factors.at[pl.ds(keep, half)]
        remote(mine, mine, back_send.at[level], back_recv.at[level], partner).start()

    def regain(level):
        half = parts >> (level + 1)
        landed(factors.at[pl.ds(0, half)], back_recv.at[level])

    barrier = pltpu.get_barrier_semaphore()
    fetch(wg, ag, 0, wbuf, abuf, in_sem, 0)
    fetch(wg, ag, 1, wbuf, abuf, in_sem, 1)
    pltpu.make_async_copy(rw, rwbuf, small.at[0]).start()
    pltpu.make_async_copy(gain, gainbuf, small.at[1]).start()

    @pl.loop(1, parts)
    def _(k):
        pl.semaphore_signal(barrier, inc=1, device_id={"rows": peer(k)}, device_id_type=MESH)

    for k in range(1, owners):
        pl.semaphore_signal(barrier, inc=1, device_id={"owner": lax.rem(own + k, owners)}, device_id_type=MESH)

    for unit in range(HEAD):
        fetched(wg, ag, unit, wbuf, abuf, in_sem, unit)
        for later in range(2 * unit + HEAD, 2 * unit + HEAD + 2):
            fetch(wg, ag, later, wbuf, abuf, in_sem, later)
        columns_sum(unit, put_head(unit))

    landed(rwbuf, small.at[0])
    landed(gainbuf, small.at[1])
    piece[...] = (rwbuf[...] * gainbuf[...]).astype(piece.dtype)
    pl.semaphore_wait(barrier, parts - 1 + owners - 1)

    @pl.loop(1, parts)
    def _(k):
        remote(direct.at[me], direct.at[me], direct_send, direct_recv, peer(k)).start()

    for later in range(3 * HEAD, EARLY):
        fetch(wg, ag, later, wbuf, abuf, in_sem, later)
    strip = router.at[own, :, pl.ds(pl.multiple_of(me * high, high), high)]

    @pl.loop(1, parts)
    def _(k):
        remote(piece, strip, piece_send, piece_recv, peer(k)).start()

    @pl.loop(HEAD, EARLY)
    def _(unit):
        fetched(wg, ag, unit, wbuf, abuf, in_sem, unit)
        columns_sum(unit, put_in(early, unit))

    landed(direct.at[pl.ds(0, parts - 1)], direct_recv)
    total = direct[0]
    for source in range(1, parts):
        total = total + direct[source]
    near[...] = 1.0 / jnp.sqrt(total)
    columns_norm(lambda s: near[0, pl.ds(s, 1), :], 0, 0, sg)

    @pl.loop(1, parts)
    def _(k):
        remote(early.at[mirrored(peer(k))], early_heard.at[me], early_send.at[0], early_recv.at[0], peer(k)).start()

    push(0, 0)
    columns_norm(lambda s: near[1, pl.ds(s, 1), :], 1, 1, sg)
    landed(early_heard.at[pl.ds(0, parts - 1)], early_recv.at[0])
    mine = mirrored(me)
    total = early[mine]
    for k in range(1, parts):
        total = total + early_heard[peer(k)]
    scale = jnp.sqrt(total)
    scales[0:EARLY] = scale
    early_factors[mine] = 1.0 / scale

    @pl.loop(1, parts)
    def _(k):
        ref = early_factors.at[mine]
        remote(ref, ref, early_send.at[1], early_recv.at[1], peer(k)).start()

    router[own, :, pl.ds(pl.multiple_of(me * high, high), high)] = piece[...]
    push(0, 1)

    first_up, first_down = experts - EARLY, 2 * experts - EARLY
    stream(
        wg, ag, wbuf, abuf, in_sem, EARLY, EARLY, experts - EARLY,
        lambda e, slot: columns_sum(slot, put_in(rest, e - EARLY)),
    )
    stream(
        wu, au, wbuf, abuf, in_sem, EARLY, 0, experts,
        lambda e, slot: columns_sum(slot, put_in(rest, first_up + e)),
    )
    landed(early_factors.at[pl.ds(0, parts - 1)], early_recv.at[1])

    @pl.loop(HEAD, EARLY)
    def _(unit):
        columns_norm(taken(early_factors, unit), unit, unit, sg)

    push(0, HEAD)
    push(0, HEAD + 1)
    stream(
        wd, ad, wdbuf, adbuf, down_sem, 0, 0, experts,
        lambda e, slot: rows_sum(slot, put_in(rest, first_down + e)),
    )
    give(0)
    gain_level(0)
    sent = HEAD + 2
    for level in range(1, levels):
        give(level)
        push(0, sent)
        sent += 1
        gain_level(level)
    keep = span(levels - 1)[0]
    scale = jnp.sqrt(rest[keep])
    scales[EARLY:] = scale
    factors[keep] = 1.0 / scale
    pltpu.make_async_copy(scales, oscale, small.at[0]).start()
    for level in range(levels - 1, 0, -1):
        back(level)
        push(0, sent)
        sent += 1
        regain(level)
    for left in range(sent, EARLY):
        push(0, left)
    back(0)
    regain(0)

    def gate(e, slot):
        columns_norm(taken(factors, e - EARLY), e, slot, sg)

        @pl.when(e > EARLY)
        def _():
            push(0, e - 1)

    def up(e, slot):
        columns_norm(taken(factors, first_up + e), e, slot, su)

        @pl.when(e > 0)
        def _():
            push(1, e - 1)

    def down(e, slot):
        rows_norm(taken(factors, first_down + e), e, slot)

        @pl.when((e > 0) & (e <= experts - tail))
        def _():
            push(2, e - 1)

    stream(wg, ag, wbuf, abuf, in_sem, EARLY, EARLY, experts - EARLY, gate)
    push(0, experts - 1)

    gathered = router.at[own, :, pl.ds(0, (parts - 1) * high)]
    landed(gathered, piece_recv)
    for k in range(1, owners):
        remote(
            router.at[own], router.at[own], router_send, router_recv, lax.rem(own + k, owners), "owner"
        ).start()

    stream(wu, au, wbuf, abuf, in_sem, EARLY, 0, experts, up)
    push(1, experts - 1)
    stream(wd, ad, wdbuf, adbuf, down_sem, 0, 0, experts, down)

    for i in range(tail):
        pltpu.make_async_copy(sd.at[experts - tail + i], ot.at[:, i], kept.at[3]).start()

    arrived = router.at[pl.ds(0, owners - 1)]
    landed(arrived, router_recv)
    pltpu.make_async_copy(router, orouter, small.at[1]).start()

    landed(direct.at[pl.ds(0, parts - 1)], direct_send)
    landed(early.at[pl.ds(0, parts - 1)], early_send.at[0])
    landed(early.at[pl.ds(0, parts - 1)], early_send.at[1])
    for level in range(levels):
        half = rest.at[pl.ds(0, parts >> (level + 1))]
        landed(half, give_send.at[level])
        landed(half, back_send.at[level])
    landed(gathered, piece_send)
    landed(arrived, router_send)
    pltpu.make_async_copy(scales, oscale, small.at[0]).wait()
    pltpu.make_async_copy(router, orouter, small.at[1]).wait()
    landed(sd.at[pl.ds(experts - tail, tail)], kept.at[3])
    for kind, send in enumerate((sg, su, sd)):
        count = experts - tail if kind == 2 else experts
        landed(send.at[pl.ds(0, count), 0], kept.at[kind])
        most = send.at[pl.ds(0, count), pl.ds(0, parts - 1)]
        landed(most, data_send.at[kind])
        landed(most, data_recv.at[kind])


def publish(depth, sg, su, sd, scale, router, og, ou, od, o1, o2, o3, orouter, tall, flat, sbuf, rbuf, load, store, small):
    slots = tall.shape[0]
    experts = og.shape[0]
    jobs = [(stage, out, tall, e) for stage, out in ((sg, og), (su, ou)) for e in range(experts)]
    jobs += [(sd, od, flat, e) for e in range(od.shape[0] - TAIL)]

    def read(i):
        stage, _, buffer, e = jobs[i]
        return pltpu.make_async_copy(stage.at[e], buffer.at[i % slots], load.at[i % slots])

    def write(i):
        _, out, buffer, e = jobs[i]
        return pltpu.make_async_copy(buffer.at[i % slots], out.at[e], store.at[i % slots])

    extras = [pltpu.make_async_copy(scale, sbuf, small.at[0]), pltpu.make_async_copy(router, rbuf, small.at[1])]
    for copy in extras:
        copy.start()
    for i in range(len(jobs) + depth):
        if i < len(jobs):
            if i >= slots:
                write(i - slots).wait()
            read(i).start()
        if i >= depth:
            read(i - depth).wait()
            write(i - depth).start()
    for copy in extras:
        copy.wait()
    outs = [pltpu.make_async_copy(sbuf.at[pl.ds(i * experts, experts)], o, small.at[2 + i]) for i, o in enumerate((o1, o2, o3))]
    columns = rbuf.shape[1]
    for i in range(rbuf.shape[0]):
        outs.append(pltpu.make_async_copy(rbuf.at[i], orouter.at[pl.ds(i * columns, columns)], small.at[5 + i]))
    for copy in outs:
        copy.start()
    for i in range(max(0, len(jobs) - slots), len(jobs)):
        write(i).wait()
    for copy in outs:
        copy.wait()


def stack_columns(x, *refs):
    o = refs[-1]
    deep = x.shape[2]
    for source in range(x.shape[0]):
        o[:, source * deep : (source + 1) * deep] = x[source]


def shards(parts, owners, w_gate, avg_gate, w_up, avg_up, w_down, avg_down, router_weight, router_gain):
    experts, high, wide = w_gate.shape
    tall, deep = w_down.shape[1:]
    block, slab = wide // parts, tall // parts
    units, slots, later = 3 * experts, EARLY + RING, 3 * experts - EARLY
    columns, model = router_weight.shape[1], parts * high
    levels = parts.bit_length() - 1
    f32, bf16 = jnp.float32, jnp.bfloat16
    any_spec = pl.BlockSpec(memory_space=pl.ANY)
    shape_columns, shape_down = (experts, high * parts, block), (experts, slab, deep * parts)
    dma = pltpu.SemaphoreType.DMA

    *stages, last, scales, routers = pl.pallas_call(
        functools.partial(regroup, parts, owners),
        in_specs=[any_spec] * 8,
        out_specs=[any_spec] * 6,
        out_shape=[
            jax.ShapeDtypeStruct(shape_columns, bf16),
            jax.ShapeDtypeStruct(shape_columns, bf16),
            jax.ShapeDtypeStruct(shape_down, bf16),
            jax.ShapeDtypeStruct((parts, TAIL, slab, deep), bf16),
            jax.ShapeDtypeStruct((units, LANES), f32),
            jax.ShapeDtypeStruct((owners, columns, model), bf16),
        ],
        scratch_shapes=[
            pltpu.VMEM((slots, high, wide), f32),
            pltpu.VMEM((slots, high, wide), bf16),
            pltpu.VMEM((RING, tall, deep), f32),
            pltpu.VMEM((RING, tall, deep), bf16),
            pltpu.VMEM((experts, parts, high, block), bf16),
            pltpu.VMEM((experts, parts, high, block), bf16),
            pltpu.VMEM((experts, parts, slab, deep), bf16),
            pltpu.VMEM((parts, HEAD, parts, LANES), f32),
            pltpu.VMEM((HEAD, parts, LANES), f32),
            pltpu.VMEM((parts, EARLY, LANES), f32),
            pltpu.VMEM((parts, EARLY, LANES), f32),
            pltpu.VMEM((parts, EARLY, LANES), f32),
            pltpu.VMEM((parts, later, LANES), f32),
            pltpu.VMEM((parts - 1, later, LANES), f32),
            pltpu.VMEM((parts, later, LANES), f32),
            pltpu.VMEM((units, LANES), f32),
            pltpu.VMEM((columns, high), f32),
            pltpu.VMEM((1, high), f32),
            pltpu.VMEM((columns, high), bf16),
            pltpu.VMEM((owners, columns, model), bf16),
            dma((2, slots)), dma((2, RING)), dma, dma, dma((2,)), dma((2,)),
            dma((levels,)), dma((levels,)), dma((levels,)), dma((levels,)),
            dma((3,)), dma((3,)), dma((4,)), dma, dma, dma, dma, dma((2,)),
        ],
        cost_estimate=pl.CostEstimate(flops=2**30, bytes_accessed=2**28, transcendentals=0),
        compiler_params=pltpu.CompilerParams(
            collective_id=0, has_side_effects=True, vmem_limit_bytes=60 * 2**20
        ),
    )(w_gate, avg_gate, w_up, avg_up, w_down, avg_down, router_weight.T, router_gain.reshape(1, high))

    got = lax.all_to_all(last, "rows", split_axis=0, concat_axis=0, tiled=True)
    serve_gate, serve_up, held, scale_gate, scale_up, scale_down, serve_router = pl.pallas_call(
        functools.partial(publish, 8),
        in_specs=[any_spec] * 5,
        out_specs=[any_spec] * 7,
        out_shape=[
            jax.ShapeDtypeStruct(shape_columns, bf16),
            jax.ShapeDtypeStruct(shape_columns, bf16),
            jax.ShapeDtypeStruct(shape_down, bf16),
            *[jax.ShapeDtypeStruct((experts, LANES), f32)] * 3,
            jax.ShapeDtypeStruct((owners * columns, model), bf16),
        ],
        scratch_shapes=[
            pltpu.VMEM((16,) + shape_columns[1:], bf16),
            pltpu.VMEM((16,) + shape_down[1:], bf16),
            pltpu.VMEM((units, LANES), f32),
            pltpu.VMEM((owners, columns, model), bf16),
            dma((16,)), dma((16,)), dma((5 + owners,)),
        ],
        cost_estimate=pl.CostEstimate(flops=2**26, bytes_accessed=2**26, transcendentals=0),
        compiler_params=pltpu.CompilerParams(vmem_limit_bytes=40 * 2**20),
    )(*stages, scales, routers)
    serve_down = pl.pallas_call(
        stack_columns,
        grid=(TAIL,),
        in_specs=[pl.BlockSpec((parts, None, slab, deep), lambda e: (0, e, 0, 0)), any_spec],
        out_specs=pl.BlockSpec((None,) + shape_down[1:], lambda e: (experts - TAIL + e, 0, 0)),
        out_shape=jax.ShapeDtypeStruct(shape_down, bf16),
        input_output_aliases={1: 0},
        cost_estimate=pl.CostEstimate(flops=2**21, bytes_accessed=2**22, transcendentals=0),
        compiler_params=pltpu.CompilerParams(vmem_limit_bytes=16 * 2**20),
    )(got, held)
    return (serve_gate, serve_up, serve_down, scale_gate, scale_up, scale_down, serve_router.T)


def plain_shards(w_gate, avg_gate, w_up, avg_up, w_down, avg_down, router_weight, router_gain):
    def served(w, a, axis, split):
        fresh = w + a.astype(jnp.float32)
        scale = jnp.sqrt(lax.psum(jnp.sum(fresh * fresh, axis=axis), "rows"))
        narrow = (fresh / jnp.expand_dims(scale, axis)).astype(jnp.bfloat16)
        serve = lax.all_to_all(narrow, "rows", split_axis=split, concat_axis=axis, tiled=True)
        width = serve.shape[split]
        return serve, lax.dynamic_slice_in_dim(scale, lax.axis_index("rows") * width, width, axis=1)

    serve_gate, scale_gate = served(w_gate, avg_gate, 1, 2)
    serve_up, scale_up = served(w_up, avg_up, 1, 2)
    serve_down, scale_down = served(w_down, avg_down, 2, 1)
    part_router = (router_weight * router_gain[:, None]).astype(jnp.bfloat16)
    row_router = lax.all_gather(part_router, "rows", axis=0, tiled=True)
    serve_router = lax.all_gather(row_router, "owner", axis=1, tiled=True)
    return (serve_gate, serve_up, serve_down, scale_gate, scale_up, scale_down, serve_router)


def solution(mesh):
    parts, owners = mesh.shape["rows"], mesh.shape["owner"]

    def dispatched(*args):
        experts, high, wide = args[0].shape
        tall, deep = args[4].shape[1:]
        block, slab = wide // parts, tall // parts
        columns = args[6].shape[1]
        aligned = block == LANES and slab == LANES and deep % LANES == 0 and high % LANES == 0
        aligned = aligned and high <= 256 and deep <= 256 and experts <= 16 and experts % 8 == 0
        aligned = aligned and experts > EARLY and columns % 16 == 0 and parts == 8 and owners > 1
        return shards(parts, owners, *args) if aligned else plain_shards(*args)

    return jax.shard_map(
        dispatched,
        mesh=mesh,
        in_specs=(
            P("owner", "rows", None),
            P("owner", "rows", None),
            P("owner", "rows", None),
            P("owner", "rows", None),
            P("owner", None, "rows"),
            P("owner", None, "rows"),
            P("rows", "owner"),
            P("rows"),
        ),
        out_specs=(
            P("owner", None, "rows"),
            P("owner", None, "rows"),
            P("owner", "rows", None),
            P("owner", "rows"),
            P("owner", "rows"),
            P("owner", "rows"),
            P(),
        ),
        check_vma=False,
    )
```

```python
import functools

import jax
import jax.numpy as jnp
from jax import lax
from jax.experimental import pallas as pl
from jax.experimental.pallas import tpu as pltpu
from jax.sharding import PartitionSpec as P

LANES = 128
EARLY = 8
RING = 4
TAIL = 3
MESH = pl.DeviceIdType.MESH


def remote(src, dst, send, recv, peer, axis="rows"):
    return pltpu.make_async_remote_copy(
        src_ref=src, dst_ref=dst, send_sem=send, recv_sem=recv, device_id={axis: peer}, device_id_type=MESH
    )


def regroup(
    parts, owners,
    wg, ag, wu, au, wd, ad, rw, gain,
    og, ou, od, *refs,
):
    ot, (oscale, orouter, *refs) = refs[:parts], refs[parts:]
    (
    wbuf, abuf, wdbuf, adbuf, sg, su, sd, direct, near, early, early_heard, early_factors,
    rest, rest_heard, factors, scales, rwbuf, gainbuf, router,
    in_sem, down_sem, direct_send, direct_recv, early_send, early_recv, give_send, give_recv, back_send, back_recv,
    data_send, data_recv, kept, strip_send, strip_recv, router_send, router_recv, small,
    ) = refs
    me = lax.axis_index("rows")
    own = lax.axis_index("owner")
    experts, high = wg.shape[0], wg.shape[1]
    deep = wd.shape[2]
    tail = ot[0].shape[0]
    levels = parts.bit_length() - 1
    bits = [lax.rem(me // 2**level, 2) for level in range(levels)]

    def peer(k):
        return lax.rem(me + k, parts)

    def mirrored(index):
        return sum(lax.rem(index // 2**i, 2) * 2 ** (levels - 1 - i) for i in range(levels))

    def fetch(w, a, e, wv, av, sem, slot):
        pltpu.make_async_copy(w.at[e], wv.at[slot], sem.at[0, slot]).start()
        pltpu.make_async_copy(a.at[e], av.at[slot], sem.at[1, slot]).start()

    def fetched(w, a, e, wv, av, sem, slot):
        pltpu.make_async_copy(w.at[e], wv.at[slot], sem.at[0, slot]).wait()
        pltpu.make_async_copy(a.at[e], av.at[slot], sem.at[1, slot]).wait()

    def landed(ref, sem):
        pltpu.make_async_copy(ref, ref, sem).wait()

    def stream(w, a, wv, av, sem, base, first, count, body):
        for i in range(min(RING - 1, count)):
            fetch(w, a, first + i, wv, av, sem, base + i)

        @pl.loop(0, count)
        def _(i):
            slot = base + lax.rem(i, RING)
            fetched(w, a, first + i, wv, av, sem, slot)

            @pl.when(i + RING - 1 < count)
            def _():
                fetch(w, a, first + i + RING - 1, wv, av, sem, base + lax.rem(i + RING - 1, RING))

            body(first + i, slot)

    def lanes(p):
        return pl.ds(pl.multiple_of(p * LANES, LANES), LANES)

    def columns_sum(slot, put):
        @pl.loop(0, parts)
        def _(s):
            p = mirrored(s)
            fresh = wbuf[slot, :, lanes(p)] + abuf[slot, :, lanes(p)].astype(jnp.float32)
            put(s, jnp.sum(fresh * fresh, axis=0, keepdims=True))

    def rows_sum(slot, put):
        @pl.loop(0, parts)
        def _(s):
            p = mirrored(s)
            fresh = wdbuf[slot, lanes(p), :] + adbuf[slot, lanes(p), :].astype(jnp.float32)
            square = fresh * fresh
            folded = square[:, :LANES]
            for start in range(LANES, deep, LANES):
                folded = folded + square[:, start : start + LANES]
            put(s, jnp.sum(folded.T, axis=0, keepdims=True))

    def columns_norm(take, e, slot, send, first=0, count=high):
        rows = pl.ds(first, count)

        @pl.loop(0, parts)
        def _(s):
            p = mirrored(s)
            fresh = wbuf[slot, rows, lanes(p)] + abuf[slot, rows, lanes(p)].astype(jnp.float32)
            send[e, p, rows, :] = (fresh * take(s)).astype(send.dtype)

    def rows_norm(take, e, slot):
        @pl.loop(0, parts)
        def _(s):
            p = mirrored(s)
            factor = jnp.broadcast_to(take(s), (LANES, LANES)).T
            for start in range(0, deep, LANES):
                fresh = wdbuf[slot, lanes(p), start : start + LANES]
                fresh = fresh + adbuf[slot, lanes(p), start : start + LANES].astype(jnp.float32)
                sd[e, p, :, start : start + LANES] = (fresh * factor).astype(sd.dtype)

    def put_first(s, row):
        direct[me, pl.ds(s, 1), :] = row
        early[s, 0:1, :] = row

    def put_in(ref, row):
        def put(s, value):
            ref[s, pl.ds(row, 1), :] = value

        return put

    def taken(ref, row):
        return lambda s: ref[s, pl.ds(row, 1), :]

    def push(kind, e):
        send, stage = ((sg, og), (su, ou), (sd, od))[kind]
        if kind < 2:
            place = stage.at[e, pl.ds(pl.multiple_of(me * high, high), high), :]
        else:
            place = stage.at[e, :, pl.ds(pl.multiple_of(me * deep, deep), deep)]

        @pl.loop(1, parts)
        def _(k):
            remote(send.at[e, peer(k)], place, data_send.at[kind], data_recv.at[kind], peer(k)).start()

        pltpu.make_async_copy(send.at[e, me], place, kept.at[kind]).start()

    def push_first(half):
        rows = pl.ds(half * (high // 2), high // 2)
        place = og.at[0, pl.ds(pl.multiple_of(me * high + half * (high // 2), high // 2), high // 2), :]

        @pl.loop(1, parts)
        def _(k):
            remote(sg.at[0, peer(k), rows, :], place, data_send.at[0], data_recv.at[0], peer(k)).start()

        pltpu.make_async_copy(sg.at[0, me, rows, :], place, kept.at[0]).start()

    def partner(level):
        return me + (1 - 2 * bits[level]) * 2**level

    def strip(block):
        return router.at[own, :, pl.ds(pl.multiple_of(block * high, high), high)]

    def strips_out(level):
        blocks = [me]
        for further in range(levels - 1, level, -1):
            blocks = blocks + [b + (1 - 2 * bits[further]) * 2**further for b in blocks]
        for block in blocks:
            remote(strip(block), strip(block), strip_send.at[level], strip_recv.at[level], partner(level)).start()

    def strips_in(level):
        landed(router.at[own, :, pl.ds(0, (parts >> (level + 1)) * high)], strip_recv.at[level])

    def span(level):
        half = parts >> (level + 1)
        start = sum(bits[i] * (parts >> (i + 1)) for i in range(level))
        return start + bits[level] * half, start + (1 - bits[level]) * half, half

    def heard(level):
        return rest_heard.at[pl.ds(parts - (parts >> level), parts >> (level + 1))]

    def give(level):
        _, away, half = span(level)
        remote(
            rest.at[pl.ds(away, half)], heard(level), give_send.at[level], give_recv.at[level], partner(level)
        ).start()

    def gain_level(level):
        keep, _, half = span(level)
        landed(heard(level), give_recv.at[level])
        first = parts - (parts >> level)
        for i in range(half):
            rest[keep + i] = rest[keep + i] + rest_heard[first + i]

    def back(level):
        keep, _, half = span(level)
        mine = factors.at[pl.ds(keep, half)]
        remote(mine, mine, back_send.at[level], back_recv.at[level], partner(level)).start()

    def regain(level):
        half = parts >> (level + 1)
        landed(factors.at[pl.ds(0, half)], back_recv.at[level])

    barrier = pltpu.get_barrier_semaphore()
    fetch(wg, ag, 0, wbuf, abuf, in_sem, 0)
    fetch(wg, ag, 1, wbuf, abuf, in_sem, 1)
    pltpu.make_async_copy(rw, rwbuf, small.at[0]).start()
    pltpu.make_async_copy(gain, gainbuf, small.at[1]).start()

    @pl.loop(1, parts)
    def _(k):
        pl.semaphore_signal(barrier, inc=1, device_id={"rows": peer(k)}, device_id_type=MESH)

    for k in range(1, owners):
        pl.semaphore_signal(barrier, inc=1, device_id={"owner": lax.rem(own + k, owners)}, device_id_type=MESH)

    fetched(wg, ag, 0, wbuf, abuf, in_sem, 0)
    for later in (2, 3):
        fetch(wg, ag, later, wbuf, abuf, in_sem, later)
    columns_sum(0, put_first)
    landed(rwbuf, small.at[0])
    landed(gainbuf, small.at[1])
    router[own, :, pl.ds(pl.multiple_of(me * high, high), high)] = (rwbuf[...] * gainbuf[...]).astype(router.dtype)
    pl.semaphore_wait(barrier, parts - 1 + owners - 1)

    @pl.loop(1, parts)
    def _(k):
        remote(direct.at[me], direct.at[me], direct_send, direct_recv, peer(k)).start()

    strips_out(levels - 1)
    for later in range(4, EARLY):
        fetch(wg, ag, later, wbuf, abuf, in_sem, later)

    @pl.loop(1, EARLY)
    def _(unit):
        fetched(wg, ag, unit, wbuf, abuf, in_sem, unit)
        columns_sum(unit, put_in(early, unit))

    landed(direct.at[pl.ds(0, parts - 1)], direct_recv)
    total = direct[0]
    for source in range(1, parts):
        total = total + direct[source]
    near[...] = 1.0 / jnp.sqrt(total)

    def first_factor(s):
        return near[pl.ds(s, 1), :]

    columns_norm(first_factor, 0, 0, sg, 0, high // 2)

    @pl.loop(1, parts)
    def _(k):
        remote(early.at[mirrored(peer(k))], early_heard.at[me], early_send.at[0], early_recv.at[0], peer(k)).start()

    push_first(0)
    columns_norm(first_factor, 0, 0, sg, high // 2, high // 2)
    landed(early_heard.at[pl.ds(0, parts - 1)], early_recv.at[0])
    mine = mirrored(me)
    total = early[mine]
    for k in range(1, parts):
        total = total + early_heard[peer(k)]
    scale = jnp.sqrt(total)
    scales[0:EARLY] = scale
    early_factors[mine] = 1.0 / scale

    @pl.loop(1, parts)
    def _(k):
        ref = early_factors.at[mine]
        remote(ref, ref, early_send.at[1], early_recv.at[1], peer(k)).start()

    push_first(1)
    first_up, first_down = experts - EARLY, 2 * experts - EARLY
    stream(
        wg, ag, wbuf, abuf, in_sem, EARLY, EARLY, experts - EARLY,
        lambda e, slot: columns_sum(slot, put_in(rest, e - EARLY)),
    )
    landed(early_factors.at[pl.ds(0, parts - 1)], early_recv.at[1])

    @pl.loop(1, 3)
    def _(unit):
        columns_norm(taken(early_factors, unit), unit, unit, sg)

    push(0, 1)

    @pl.loop(3, EARLY)
    def _(unit):
        columns_norm(taken(early_factors, unit), unit, unit, sg)

    push(0, 2)
    for level in range(levels - 1, 1, -1):
        strips_in(level)
        strips_out(level - 1)
    stream(
        wu, au, wbuf, abuf, in_sem, EARLY, 0, experts,
        lambda e, slot: columns_sum(slot, put_in(rest, first_up + e)),
    )
    push(0, 3)
    stream(
        wd, ad, wdbuf, adbuf, down_sem, 0, 0, experts,
        lambda e, slot: rows_sum(slot, put_in(rest, first_down + e)),
    )
    give(0)
    strips_in(1)
    strips_out(0)
    gain_level(0)
    sent = 4
    for level in range(1, levels):
        give(level)
        push(0, sent)
        sent += 1
        gain_level(level)
    keep = span(levels - 1)[0]
    scale = jnp.sqrt(rest[keep])
    scales[EARLY:] = scale
    factors[keep] = 1.0 / scale
    pltpu.make_async_copy(scales, oscale, small.at[0]).start()
    for level in range(levels - 1, 0, -1):
        back(level)
        push(0, sent)
        sent += 1
        regain(level)
    for left in range(sent, EARLY):
        push(0, left)
    back(0)
    regain(0)

    def gate(e, slot):
        columns_norm(taken(factors, e - EARLY), e, slot, sg)

        @pl.when(e > EARLY)
        def _():
            push(0, e - 1)

    def up(e, slot):
        columns_norm(taken(factors, first_up + e), e, slot, su)

        @pl.when(e > 0)
        def _():
            push(1, e - 1)

    def down(e, slot):
        rows_norm(taken(factors, first_down + e), e, slot)

        @pl.when((e > 0) & (e <= experts - tail))
        def _():
            push(2, e - 1)

    stream(wg, ag, wbuf, abuf, in_sem, EARLY, EARLY, experts - EARLY, gate)
    push(0, experts - 1)

    strips_in(0)
    for k in range(1, owners):
        remote(
            router.at[own], router.at[own], router_send, router_recv, lax.rem(own + k, owners), "owner"
        ).start()

    stream(wu, au, wbuf, abuf, in_sem, EARLY, 0, experts, up)
    push(1, experts - 1)
    stream(wd, ad, wdbuf, adbuf, down_sem, 0, 0, experts, down)

    for k in range(parts):
        pltpu.make_async_copy(sd.at[pl.ds(experts - tail, tail), peer(k)], ot[k], kept.at[3]).start()

    arrived = router.at[pl.ds(0, owners - 1)]
    landed(arrived, router_recv)
    pltpu.make_async_copy(router, orouter, small.at[1]).start()

    landed(direct.at[pl.ds(0, parts - 1)], direct_send)
    landed(early.at[pl.ds(0, parts - 1)], early_send.at[0])
    landed(early.at[pl.ds(0, parts - 1)], early_send.at[1])
    for level in range(levels):
        half = rest.at[pl.ds(0, parts >> (level + 1))]
        landed(half, give_send.at[level])
        landed(half, back_send.at[level])
        landed(router.at[own, :, pl.ds(0, (parts >> (level + 1)) * high)], strip_send.at[level])
    landed(arrived, router_send)
    pltpu.make_async_copy(scales, oscale, small.at[0]).wait()
    pltpu.make_async_copy(router, orouter, small.at[1]).wait()
    landed(sd.at[pl.ds(experts - tail, tail)], kept.at[3])
    for kind, send in enumerate((sg, su, sd)):
        count = experts - tail if kind == 2 else experts
        landed(send.at[pl.ds(0, count), 0], kept.at[kind])
        most = send.at[pl.ds(0, count), pl.ds(0, parts - 1)]
        landed(most, data_send.at[kind])
        landed(most, data_recv.at[kind])


def publish(depth, sg, su, sd, scale, router, og, ou, od, o1, o2, o3, orouter, tall, flat, sbuf, rbuf, load, store, small):
    slots = tall.shape[0]
    experts = og.shape[0]
    jobs = [(stage, out, tall, e) for stage, out in ((sg, og), (su, ou)) for e in range(experts)]
    jobs += [(sd, od, flat, e) for e in range(od.shape[0] - TAIL)]

    def read(i):
        stage, _, buffer, e = jobs[i]
        return pltpu.make_async_copy(stage.at[e], buffer.at[i % slots], load.at[i % slots])

    def write(i):
        _, out, buffer, e = jobs[i]
        return pltpu.make_async_copy(buffer.at[i % slots], out.at[e], store.at[i % slots])

    extras = [pltpu.make_async_copy(scale, sbuf, small.at[0]), pltpu.make_async_copy(router, rbuf, small.at[1])]
    for copy in extras:
        copy.start()
    for i in range(len(jobs) + depth):
        if i < len(jobs):
            if i >= slots:
                write(i - slots).wait()
            read(i).start()
        if i >= depth:
            read(i - depth).wait()
            write(i - depth).start()
    for copy in extras:
        copy.wait()
    outs = [pltpu.make_async_copy(sbuf.at[pl.ds(i * experts, experts)], o, small.at[2 + i]) for i, o in enumerate((o1, o2, o3))]
    columns = rbuf.shape[1]
    for i in range(rbuf.shape[0]):
        outs.append(pltpu.make_async_copy(rbuf.at[i], orouter.at[pl.ds(i * columns, columns)], small.at[5 + i]))
    for copy in outs:
        copy.start()
    for i in range(max(0, len(jobs) - slots), len(jobs)):
        write(i).wait()
    for copy in outs:
        copy.wait()


def stack_columns(*refs):
    *xs, _, o, sem = refs
    me, parts = lax.axis_index("rows"), len(xs)
    tail, _, deep = xs[0].shape
    copies = []
    for k, x in enumerate(xs):
        source = lax.rem(me + parts - k, parts)
        place = o.at[pl.ds(o.shape[0] - tail, tail), :, pl.ds(pl.multiple_of(source * deep, deep), deep)]
        copies.append(pltpu.make_async_copy(x, place, sem.at[k]))
    for copy in copies:
        copy.start()
    for copy in copies:
        copy.wait()


def shards(parts, owners, w_gate, avg_gate, w_up, avg_up, w_down, avg_down, router_weight, router_gain):
    experts, high, wide = w_gate.shape
    tall, deep = w_down.shape[1:]
    block, slab = wide // parts, tall // parts
    units, slots, later = 3 * experts, EARLY + RING, 3 * experts - EARLY
    columns, model = router_weight.shape[1], parts * high
    levels = parts.bit_length() - 1
    f32, bf16 = jnp.float32, jnp.bfloat16
    any_spec = pl.BlockSpec(memory_space=pl.ANY)
    shape_columns, shape_down = (experts, high * parts, block), (experts, slab, deep * parts)
    dma = pltpu.SemaphoreType.DMA

    *stages, scales, routers = pl.pallas_call(
        functools.partial(regroup, parts, owners),
        in_specs=[any_spec] * 8,
        out_specs=[any_spec] * (5 + parts),
        out_shape=[
            jax.ShapeDtypeStruct(shape_columns, bf16),
            jax.ShapeDtypeStruct(shape_columns, bf16),
            jax.ShapeDtypeStruct(shape_down, bf16),
            *[jax.ShapeDtypeStruct((TAIL, slab, deep), bf16)] * parts,
            jax.ShapeDtypeStruct((units, LANES), f32),
            jax.ShapeDtypeStruct((owners, columns, model), bf16),
        ],
        scratch_shapes=[
            pltpu.VMEM((slots, high, wide), f32),
            pltpu.VMEM((slots, high, wide), bf16),
            pltpu.VMEM((RING, tall, deep), f32),
            pltpu.VMEM((RING, tall, deep), bf16),
            pltpu.VMEM((experts, parts, high, block), bf16),
            pltpu.VMEM((experts, parts, high, block), bf16),
            pltpu.VMEM((experts, parts, slab, deep), bf16),
            pltpu.VMEM((parts, parts, LANES), f32),
            pltpu.VMEM((parts, LANES), f32),
            pltpu.VMEM((parts, EARLY, LANES), f32),
            pltpu.VMEM((parts, EARLY, LANES), f32),
            pltpu.VMEM((parts, EARLY, LANES), f32),
            pltpu.VMEM((parts, later, LANES), f32),
            pltpu.VMEM((parts - 1, later, LANES), f32),
            pltpu.VMEM((parts, later, LANES), f32),
            pltpu.VMEM((units, LANES), f32),
            pltpu.VMEM((columns, high), f32),
            pltpu.VMEM((1, high), f32),
            pltpu.VMEM((owners, columns, model), bf16),
            dma((2, slots)), dma((2, RING)), dma, dma, dma((2,)), dma((2,)),
            dma((levels,)), dma((levels,)), dma((levels,)), dma((levels,)),
            dma((3,)), dma((3,)), dma((4,)), dma((levels,)), dma((levels,)), dma, dma, dma((2,)),
        ],
        cost_estimate=pl.CostEstimate(flops=2**30, bytes_accessed=2**28, transcendentals=0),
        compiler_params=pltpu.CompilerParams(
            collective_id=0, has_side_effects=True, vmem_limit_bytes=60 * 2**20
        ),
    )(w_gate, avg_gate, w_up, avg_up, w_down, avg_down, router_weight.T, router_gain.reshape(1, high))

    stages, pieces = stages[:3], stages[3:]
    got = [
        lax.ppermute(x, "rows", [(i, (i + k) % parts) for i in range(parts)]) if k else x
        for k, x in enumerate(pieces)
    ]
    serve_gate, serve_up, held, scale_gate, scale_up, scale_down, serve_router = pl.pallas_call(
        functools.partial(publish, 8),
        in_specs=[any_spec] * 5,
        out_specs=[any_spec] * 7,
        out_shape=[
            jax.ShapeDtypeStruct(shape_columns, bf16),
            jax.ShapeDtypeStruct(shape_columns, bf16),
            jax.ShapeDtypeStruct(shape_down, bf16),
            *[jax.ShapeDtypeStruct((experts, LANES), f32)] * 3,
            jax.ShapeDtypeStruct((owners * columns, model), bf16),
        ],
        scratch_shapes=[
            pltpu.VMEM((16,) + shape_columns[1:], bf16),
            pltpu.VMEM((16,) + shape_down[1:], bf16),
            pltpu.VMEM((units, LANES), f32),
            pltpu.VMEM((owners, columns, model), bf16),
            dma((16,)), dma((16,)), dma((5 + owners,)),
        ],
        cost_estimate=pl.CostEstimate(flops=2**26, bytes_accessed=2**26, transcendentals=0),
        compiler_params=pltpu.CompilerParams(vmem_limit_bytes=62 * 2**20),
    )(*stages, scales, routers)
    serve_down = pl.pallas_call(
        stack_columns,
        in_specs=[pl.BlockSpec(memory_space=pltpu.VMEM)] * parts + [any_spec],
        out_specs=any_spec,
        out_shape=jax.ShapeDtypeStruct(shape_down, bf16),
        scratch_shapes=[dma((parts,))],
        input_output_aliases={parts: 0},
        cost_estimate=pl.CostEstimate(flops=2**21, bytes_accessed=2**22, transcendentals=0),
        compiler_params=pltpu.CompilerParams(vmem_limit_bytes=16 * 2**20),
    )(*got, held)
    return (serve_gate, serve_up, serve_down, scale_gate, scale_up, scale_down, serve_router.T)


def plain_shards(w_gate, avg_gate, w_up, avg_up, w_down, avg_down, router_weight, router_gain):
    def served(w, a, axis, split):
        fresh = w + a.astype(jnp.float32)
        scale = jnp.sqrt(lax.psum(jnp.sum(fresh * fresh, axis=axis), "rows"))
        narrow = (fresh / jnp.expand_dims(scale, axis)).astype(jnp.bfloat16)
        serve = lax.all_to_all(narrow, "rows", split_axis=split, concat_axis=axis, tiled=True)
        width = serve.shape[split]
        return serve, lax.dynamic_slice_in_dim(scale, lax.axis_index("rows") * width, width, axis=1)

    serve_gate, scale_gate = served(w_gate, avg_gate, 1, 2)
    serve_up, scale_up = served(w_up, avg_up, 1, 2)
    serve_down, scale_down = served(w_down, avg_down, 2, 1)
    part_router = (router_weight * router_gain[:, None]).astype(jnp.bfloat16)
    row_router = lax.all_gather(part_router, "rows", axis=0, tiled=True)
    serve_router = lax.all_gather(row_router, "owner", axis=1, tiled=True)
    return (serve_gate, serve_up, serve_down, scale_gate, scale_up, scale_down, serve_router)


def solution(mesh):
    parts, owners = mesh.shape["rows"], mesh.shape["owner"]

    def dispatched(*args):
        experts, high, wide = args[0].shape
        tall, deep = args[4].shape[1:]
        block, slab = wide // parts, tall // parts
        columns = args[6].shape[1]
        aligned = block == LANES and slab == LANES and deep % LANES == 0 and high % LANES == 0
        aligned = aligned and high <= 256 and deep <= 256 and experts <= 16 and experts % 8 == 0
        aligned = aligned and experts > EARLY and columns % 16 == 0 and parts == 8 and owners > 1
        return shards(parts, owners, *args) if aligned else plain_shards(*args)

    return jax.shard_map(
        dispatched,
        mesh=mesh,
        in_specs=(
            P("owner", "rows", None),
            P("owner", "rows", None),
            P("owner", "rows", None),
            P("owner", "rows", None),
            P("owner", None, "rows"),
            P("owner", None, "rows"),
            P("rows", "owner"),
            P("rows"),
        ),
        out_specs=(
            P("owner", None, "rows"),
            P("owner", None, "rows"),
            P("owner", "rows", None),
            P("owner", "rows"),
            P("owner", "rows"),
            P("owner", "rows"),
            P(),
        ),
        check_vma=False,
    )
```

```python
import functools

import jax
import jax.numpy as jnp
from jax import lax
from jax.experimental import pallas as pl
from jax.experimental.pallas import tpu as pltpu
from jax.sharding import PartitionSpec as P

LANES = 128
EARLY = 8
RING = 4
TAIL = 3
MESH = pl.DeviceIdType.MESH


def remote(src, dst, send, recv, peer, axis="rows"):
    return pltpu.make_async_remote_copy(
        src_ref=src, dst_ref=dst, send_sem=send, recv_sem=recv, device_id={axis: peer}, device_id_type=MESH
    )


def regroup(
    parts, owners,
    wg, ag, wu, au, wd, ad, rw, gain,
    og, ou, od, *refs,
):
    ot, (oscale, orouter, *refs) = refs[:parts], refs[parts:]
    (
    wbuf, abuf, wdbuf, adbuf, sg, su, sd, direct, near, early, early_heard, early_factors,
    rest, rest_heard, factors, scales, rwbuf, gainbuf, router,
    in_sem, down_sem, direct_send, direct_recv, early_send, early_recv, give_send, give_recv, back_send, back_recv,
    data_send, data_recv, kept, strip_send, strip_recv, router_send, router_recv, small,
    ) = refs
    me = lax.axis_index("rows")
    own = lax.axis_index("owner")
    experts, high = wg.shape[0], wg.shape[1]
    deep = wd.shape[2]
    tail = ot[0].shape[0]
    levels = parts.bit_length() - 1
    bits = [lax.rem(me // 2**level, 2) for level in range(levels)]

    def peer(k):
        return lax.rem(me + k, parts)

    def mirrored(index):
        return sum(lax.rem(index // 2**i, 2) * 2 ** (levels - 1 - i) for i in range(levels))

    def fetch(w, a, e, wv, av, sem, slot):
        pltpu.make_async_copy(w.at[e], wv.at[slot], sem.at[0, slot]).start()
        pltpu.make_async_copy(a.at[e], av.at[slot], sem.at[1, slot]).start()

    def fetched(w, a, e, wv, av, sem, slot):
        pltpu.make_async_copy(w.at[e], wv.at[slot], sem.at[0, slot]).wait()
        pltpu.make_async_copy(a.at[e], av.at[slot], sem.at[1, slot]).wait()

    def landed(ref, sem):
        pltpu.make_async_copy(ref, ref, sem).wait()

    def stream(w, a, wv, av, sem, base, first, count, body):
        for i in range(min(RING - 1, count)):
            fetch(w, a, first + i, wv, av, sem, base + i)

        @pl.loop(0, count)
        def _(i):
            slot = base + lax.rem(i, RING)
            fetched(w, a, first + i, wv, av, sem, slot)

            @pl.when(i + RING - 1 < count)
            def _():
                fetch(w, a, first + i + RING - 1, wv, av, sem, base + lax.rem(i + RING - 1, RING))

            body(first + i, slot)

    def lanes(p):
        return pl.ds(pl.multiple_of(p * LANES, LANES), LANES)

    def columns_sum(slot, put):
        @pl.loop(0, parts)
        def _(s):
            p = mirrored(s)
            fresh = wbuf[slot, :, lanes(p)] + abuf[slot, :, lanes(p)].astype(jnp.float32)
            put(s, jnp.sum(fresh * fresh, axis=0, keepdims=True))

    def rows_sum(slot, put):
        @pl.loop(0, parts)
        def _(s):
            p = mirrored(s)
            fresh = wdbuf[slot, lanes(p), :] + adbuf[slot, lanes(p), :].astype(jnp.float32)
            square = fresh * fresh
            folded = square[:, :LANES]
            for start in range(LANES, deep, LANES):
                folded = folded + square[:, start : start + LANES]
            put(s, jnp.sum(folded.T, axis=0, keepdims=True))

    def columns_norm(take, e, slot, send, first=0, count=high):
        rows = pl.ds(first, count)

        @pl.loop(0, parts)
        def _(s):
            p = mirrored(s)
            fresh = wbuf[slot, rows, lanes(p)] + abuf[slot, rows, lanes(p)].astype(jnp.float32)
            send[e, p, rows, :] = (fresh * take(s)).astype(send.dtype)

    def rows_norm(take, e, slot):
        @pl.loop(0, parts)
        def _(s):
            p = mirrored(s)
            factor = jnp.broadcast_to(take(s), (LANES, LANES)).T
            for start in range(0, deep, LANES):
                fresh = wdbuf[slot, lanes(p), start : start + LANES]
                fresh = fresh + adbuf[slot, lanes(p), start : start + LANES].astype(jnp.float32)
                sd[e, p, :, start : start + LANES] = (fresh * factor).astype(sd.dtype)

    def put_first(s, row):
        direct[me, pl.ds(s, 1), :] = row
        early[s, 0:1, :] = row

    def put_in(ref, row):
        def put(s, value):
            ref[s, pl.ds(row, 1), :] = value

        return put

    def taken(ref, row):
        return lambda s: ref[s, pl.ds(row, 1), :]

    def push(kind, e):
        send, stage = ((sg, og), (su, ou), (sd, od))[kind]
        if kind < 2:
            place = stage.at[e, pl.ds(pl.multiple_of(me * high, high), high), :]
        else:
            place = stage.at[e, :, pl.ds(pl.multiple_of(me * deep, deep), deep)]

        @pl.loop(1, parts)
        def _(k):
            remote(send.at[e, peer(k)], place, data_send.at[kind], data_recv.at[kind], peer(k)).start()

        pltpu.make_async_copy(send.at[e, me], place, kept.at[kind]).start()

    def push_first(half):
        rows = pl.ds(half * (high // 2), high // 2)
        place = og.at[0, pl.ds(pl.multiple_of(me * high + half * (high // 2), high // 2), high // 2), :]

        @pl.loop(1, parts)
        def _(k):
            remote(sg.at[0, peer(k), rows, :], place, data_send.at[0], data_recv.at[0], peer(k)).start()

        pltpu.make_async_copy(sg.at[0, me, rows, :], place, kept.at[0]).start()

    def flipped(mask):
        return me + sum((1 - 2 * bits[i]) * 2**i for i in range(levels) if mask >> i & 1)

    def partner(level):
        return flipped(1 << level)

    def strip(block):
        return router.at[own, :, pl.ds(pl.multiple_of(block * high, high), high)]

    def strips_out(level):
        blocks = [me]
        for further in range(levels - 1, level, -1):
            blocks = blocks + [b + (1 - 2 * bits[further]) * 2**further for b in blocks]
        for block in blocks:
            remote(strip(block), strip(block), strip_send.at[level], strip_recv.at[level], partner(level)).start()

    def strips_in(level):
        landed(router.at[own, :, pl.ds(0, (parts >> (level + 1)) * high)], strip_recv.at[level])

    def span(level):
        half = parts >> (level + 1)
        start = sum(bits[i] * (parts >> (i + 1)) for i in range(level))
        return start + bits[level] * half, start + (1 - bits[level]) * half, half

    def heard(level):
        return rest_heard.at[pl.ds(parts - (parts >> level), parts >> (level + 1))]

    def give(level):
        _, away, half = span(level)
        remote(
            rest.at[pl.ds(away, half)], heard(level), give_send.at[level], give_recv.at[level], partner(level)
        ).start()

    def gain_level(level):
        keep, _, half = span(level)
        landed(heard(level), give_recv.at[level])
        first = parts - (parts >> level)
        for i in range(half):
            rest[keep + i] = rest[keep + i] + rest_heard[first + i]

    def back(level):
        keep, _, half = span(level)
        mine = factors.at[pl.ds(keep, half)]
        remote(mine, mine, back_send.at[level], back_recv.at[level], partner(level)).start()

    def regain(level):
        half = parts >> (level + 1)
        landed(factors.at[pl.ds(0, half)], back_recv.at[level])

    barrier = pltpu.get_barrier_semaphore()
    fetch(wg, ag, 0, wbuf, abuf, in_sem, 0)
    fetch(wg, ag, 1, wbuf, abuf, in_sem, 1)
    pltpu.make_async_copy(rw, rwbuf, small.at[0]).start()
    pltpu.make_async_copy(gain, gainbuf, small.at[1]).start()

    @pl.loop(1, parts)
    def _(k):
        pl.semaphore_signal(barrier, inc=1, device_id={"rows": peer(k)}, device_id_type=MESH)

    for k in range(1, owners):
        pl.semaphore_signal(barrier, inc=1, device_id={"owner": lax.rem(own + k, owners)}, device_id_type=MESH)

    fetched(wg, ag, 0, wbuf, abuf, in_sem, 0)
    for later in (2, 3):
        fetch(wg, ag, later, wbuf, abuf, in_sem, later)
    columns_sum(0, put_first)
    landed(rwbuf, small.at[0])
    landed(gainbuf, small.at[1])
    router[own, :, pl.ds(pl.multiple_of(me * high, high), high)] = (rwbuf[...] * gainbuf[...]).astype(router.dtype)
    pl.semaphore_wait(barrier, parts - 1 + owners - 1)

    @pl.loop(1, parts)
    def _(k):
        remote(direct.at[me], direct.at[me], direct_send, direct_recv, peer(k)).start()

    strips_out(levels - 1)
    for later in range(4, EARLY):
        fetch(wg, ag, later, wbuf, abuf, in_sem, later)

    @pl.loop(1, EARLY)
    def _(unit):
        fetched(wg, ag, unit, wbuf, abuf, in_sem, unit)
        columns_sum(unit, put_in(early, unit))

    landed(direct.at[pl.ds(0, parts - 1)], direct_recv)
    total = direct[0]
    for source in range(1, parts):
        total = total + direct[source]
    near[...] = 1.0 / jnp.sqrt(total)

    def first_factor(s):
        return near[pl.ds(s, 1), :]

    columns_norm(first_factor, 0, 0, sg, 0, high // 2)

    @pl.loop(1, parts)
    def _(k):
        remote(early.at[mirrored(peer(k))], early_heard.at[me], early_send.at[0], early_recv.at[0], peer(k)).start()

    push_first(0)
    columns_norm(first_factor, 0, 0, sg, high // 2, high // 2)
    landed(early_heard.at[pl.ds(0, parts - 1)], early_recv.at[0])
    mine = mirrored(me)
    total = early[mine]
    for k in range(1, parts):
        total = total + early_heard[peer(k)]
    scale = jnp.sqrt(total)
    scales[0:EARLY] = scale
    early_factors[mine] = 1.0 / scale

    @pl.loop(1, parts)
    def _(k):
        ref = early_factors.at[mine]
        remote(ref, ref, early_send.at[1], early_recv.at[1], peer(k)).start()

    push_first(1)
    first_up, first_down = experts - EARLY, 2 * experts - EARLY
    stream(
        wg, ag, wbuf, abuf, in_sem, EARLY, EARLY, experts - EARLY,
        lambda e, slot: columns_sum(slot, put_in(rest, e - EARLY)),
    )
    landed(early_factors.at[pl.ds(0, parts - 1)], early_recv.at[1])

    @pl.loop(1, 3)
    def _(unit):
        columns_norm(taken(early_factors, unit), unit, unit, sg)

    push(0, 1)

    @pl.loop(3, EARLY)
    def _(unit):
        columns_norm(taken(early_factors, unit), unit, unit, sg)

    push(0, 2)
    for level in range(levels - 1, 1, -1):
        strips_in(level)
        strips_out(level - 1)
    stream(
        wu, au, wbuf, abuf, in_sem, EARLY, 0, experts,
        lambda e, slot: columns_sum(slot, put_in(rest, first_up + e)),
    )
    push(0, 3)
    stream(
        wd, ad, wdbuf, adbuf, down_sem, 0, 0, experts,
        lambda e, slot: rows_sum(slot, put_in(rest, first_down + e)),
    )
    give(0)
    strips_in(1)
    strips_out(0)
    gain_level(0)
    sent = 4
    for level in range(1, levels):
        give(level)
        push(0, sent)
        sent += 1
        gain_level(level)
    keep = span(levels - 1)[0]
    scale = jnp.sqrt(rest[keep])
    scales[EARLY:] = scale
    factors[keep] = 1.0 / scale
    pltpu.make_async_copy(scales, oscale, small.at[0]).start()
    for level in range(levels - 1, 0, -1):
        back(level)
        push(0, sent)
        sent += 1
        regain(level)
    for left in range(sent, EARLY):
        push(0, left)
    back(0)
    regain(0)

    def gate(e, slot):
        columns_norm(taken(factors, e - EARLY), e, slot, sg)

        @pl.when(e > EARLY)
        def _():
            push(0, e - 1)

    def up(e, slot):
        columns_norm(taken(factors, first_up + e), e, slot, su)

        @pl.when(e > 0)
        def _():
            push(1, e - 1)

    def down(e, slot):
        rows_norm(taken(factors, first_down + e), e, slot)

        @pl.when((e > 0) & (e <= experts - tail))
        def _():
            push(2, e - 1)

    stream(wg, ag, wbuf, abuf, in_sem, EARLY, EARLY, experts - EARLY, gate)
    push(0, experts - 1)

    strips_in(0)
    for k in range(1, owners):
        remote(
            router.at[own], router.at[own], router_send, router_recv, lax.rem(own + k, owners), "owner"
        ).start()

    stream(wu, au, wbuf, abuf, in_sem, EARLY, 0, experts, up)
    push(1, experts - 1)
    stream(wd, ad, wdbuf, adbuf, down_sem, 0, 0, experts, down)

    for mask in range(parts):
        pltpu.make_async_copy(sd.at[pl.ds(experts - tail, tail), flipped(mask)], ot[mask], kept.at[3]).start()

    arrived = router.at[pl.ds(0, owners - 1)]
    landed(arrived, router_recv)
    pltpu.make_async_copy(router, orouter, small.at[1]).start()

    landed(direct.at[pl.ds(0, parts - 1)], direct_send)
    landed(early.at[pl.ds(0, parts - 1)], early_send.at[0])
    landed(early.at[pl.ds(0, parts - 1)], early_send.at[1])
    for level in range(levels):
        half = rest.at[pl.ds(0, parts >> (level + 1))]
        landed(half, give_send.at[level])
        landed(half, back_send.at[level])
        landed(router.at[own, :, pl.ds(0, (parts >> (level + 1)) * high)], strip_send.at[level])
    landed(arrived, router_send)
    pltpu.make_async_copy(scales, oscale, small.at[0]).wait()
    pltpu.make_async_copy(router, orouter, small.at[1]).wait()
    landed(sd.at[pl.ds(experts - tail, tail)], kept.at[3])
    for kind, send in enumerate((sg, su, sd)):
        count = experts - tail if kind == 2 else experts
        landed(send.at[pl.ds(0, count), 0], kept.at[kind])
        most = send.at[pl.ds(0, count), pl.ds(0, parts - 1)]
        landed(most, data_send.at[kind])
        landed(most, data_recv.at[kind])


def publish(depth, sg, su, sd, scale, router, og, ou, od, o1, o2, o3, orouter, tall, flat, sbuf, rbuf, load, store, small):
    slots = tall.shape[0]
    experts = og.shape[0]
    jobs = [(stage, out, tall, e) for stage, out in ((sg, og), (su, ou)) for e in range(experts)]
    jobs += [(sd, od, flat, e) for e in range(od.shape[0] - TAIL)]

    def read(i):
        stage, _, buffer, e = jobs[i]
        return pltpu.make_async_copy(stage.at[e], buffer.at[i % slots], load.at[i % slots])

    def write(i):
        _, out, buffer, e = jobs[i]
        return pltpu.make_async_copy(buffer.at[i % slots], out.at[e], store.at[i % slots])

    extras = [pltpu.make_async_copy(scale, sbuf, small.at[0]), pltpu.make_async_copy(router, rbuf, small.at[1])]
    for copy in extras:
        copy.start()
    for i in range(len(jobs) + depth):
        if i < len(jobs):
            if i >= slots:
                write(i - slots).wait()
            read(i).start()
        if i >= depth:
            read(i - depth).wait()
            write(i - depth).start()
    for copy in extras:
        copy.wait()
    outs = [pltpu.make_async_copy(sbuf.at[pl.ds(i * experts, experts)], o, small.at[2 + i]) for i, o in enumerate((o1, o2, o3))]
    columns = rbuf.shape[1]
    for i in range(rbuf.shape[0]):
        outs.append(pltpu.make_async_copy(rbuf.at[i], orouter.at[pl.ds(i * columns, columns)], small.at[5 + i]))
    for copy in outs:
        copy.start()
    for i in range(max(0, len(jobs) - slots), len(jobs)):
        write(i).wait()
    for copy in outs:
        copy.wait()


def stack_columns(order, *refs):
    *xs, _, o, sem = refs
    me, parts = lax.axis_index("rows"), len(xs)
    tail, _, deep = xs[0].shape
    copies = []
    for mask, x in zip(order, xs):
        source = sum(lax.rem(me // 2**i + (mask >> i & 1), 2) * 2**i for i in range(parts.bit_length() - 1))
        place = o.at[pl.ds(o.shape[0] - tail, tail), :, pl.ds(pl.multiple_of(source * deep, deep), deep)]
        copies.append(pltpu.make_async_copy(x, place, sem.at[mask]))
    for copy in copies:
        copy.start()
    for copy in copies:
        copy.wait()


def shards(parts, owners, w_gate, avg_gate, w_up, avg_up, w_down, avg_down, router_weight, router_gain):
    experts, high, wide = w_gate.shape
    tall, deep = w_down.shape[1:]
    block, slab = wide // parts, tall // parts
    units, slots, later = 3 * experts, EARLY + RING, 3 * experts - EARLY
    columns, model = router_weight.shape[1], parts * high
    levels = parts.bit_length() - 1
    f32, bf16 = jnp.float32, jnp.bfloat16
    any_spec = pl.BlockSpec(memory_space=pl.ANY)
    shape_columns, shape_down = (experts, high * parts, block), (experts, slab, deep * parts)
    dma = pltpu.SemaphoreType.DMA

    *stages, scales, routers = pl.pallas_call(
        functools.partial(regroup, parts, owners),
        in_specs=[any_spec] * 8,
        out_specs=[any_spec] * (5 + parts),
        out_shape=[
            jax.ShapeDtypeStruct(shape_columns, bf16),
            jax.ShapeDtypeStruct(shape_columns, bf16),
            jax.ShapeDtypeStruct(shape_down, bf16),
            *[jax.ShapeDtypeStruct((TAIL, slab, deep), bf16)] * parts,
            jax.ShapeDtypeStruct((units, LANES), f32),
            jax.ShapeDtypeStruct((owners, columns, model), bf16),
        ],
        scratch_shapes=[
            pltpu.VMEM((slots, high, wide), f32),
            pltpu.VMEM((slots, high, wide), bf16),
            pltpu.VMEM((RING, tall, deep), f32),
            pltpu.VMEM((RING, tall, deep), bf16),
            pltpu.VMEM((experts, parts, high, block), bf16),
            pltpu.VMEM((experts, parts, high, block), bf16),
            pltpu.VMEM((experts, parts, slab, deep), bf16),
            pltpu.VMEM((parts, parts, LANES), f32),
            pltpu.VMEM((parts, LANES), f32),
            pltpu.VMEM((parts, EARLY, LANES), f32),
            pltpu.VMEM((parts, EARLY, LANES), f32),
            pltpu.VMEM((parts, EARLY, LANES), f32),
            pltpu.VMEM((parts, later, LANES), f32),
            pltpu.VMEM((parts - 1, later, LANES), f32),
            pltpu.VMEM((parts, later, LANES), f32),
            pltpu.VMEM((units, LANES), f32),
            pltpu.VMEM((columns, high), f32),
            pltpu.VMEM((1, high), f32),
            pltpu.VMEM((owners, columns, model), bf16),
            dma((2, slots)), dma((2, RING)), dma, dma, dma((2,)), dma((2,)),
            dma((levels,)), dma((levels,)), dma((levels,)), dma((levels,)),
            dma((3,)), dma((3,)), dma((4,)), dma((levels,)), dma((levels,)), dma, dma, dma((2,)),
        ],
        cost_estimate=pl.CostEstimate(flops=2**30, bytes_accessed=2**28, transcendentals=0),
        compiler_params=pltpu.CompilerParams(
            collective_id=0, has_side_effects=True, vmem_limit_bytes=60 * 2**20
        ),
    )(w_gate, avg_gate, w_up, avg_up, w_down, avg_down, router_weight.T, router_gain.reshape(1, high))

    stages, pieces = stages[:3], stages[3:]
    order = [4, 5, 6, 7, 2, 3, 1, 0]
    got = [
        lax.ppermute(pieces[mask], "rows", [(i, i ^ mask) for i in range(parts)]) if mask else pieces[0]
        for mask in order
    ]

    serve_gate, serve_up, held, scale_gate, scale_up, scale_down, serve_router = pl.pallas_call(
        functools.partial(publish, 8),
        in_specs=[any_spec] * 5,
        out_specs=[any_spec] * 7,
        out_shape=[
            jax.ShapeDtypeStruct(shape_columns, bf16),
            jax.ShapeDtypeStruct(shape_columns, bf16),
            jax.ShapeDtypeStruct(shape_down, bf16),
            *[jax.ShapeDtypeStruct((experts, LANES), f32)] * 3,
            jax.ShapeDtypeStruct((owners * columns, model), bf16),
        ],
        scratch_shapes=[
            pltpu.VMEM((16,) + shape_columns[1:], bf16),
            pltpu.VMEM((16,) + shape_down[1:], bf16),
            pltpu.VMEM((units, LANES), f32),
            pltpu.VMEM((owners, columns, model), bf16),
            dma((16,)), dma((16,)), dma((5 + owners,)),
        ],
        cost_estimate=pl.CostEstimate(flops=2**26, bytes_accessed=2**26, transcendentals=0),
        compiler_params=pltpu.CompilerParams(vmem_limit_bytes=62 * 2**20),
    )(*stages, scales, routers)
    serve_down = pl.pallas_call(
        functools.partial(stack_columns, order),
        in_specs=[pl.BlockSpec(memory_space=pltpu.VMEM)] * parts + [any_spec],
        out_specs=any_spec,
        out_shape=jax.ShapeDtypeStruct(shape_down, bf16),
        scratch_shapes=[dma((parts,))],
        input_output_aliases={parts: 0},
        cost_estimate=pl.CostEstimate(flops=2**21, bytes_accessed=2**22, transcendentals=0),
        compiler_params=pltpu.CompilerParams(vmem_limit_bytes=16 * 2**20),
    )(*got, held)
    return (serve_gate, serve_up, serve_down, scale_gate, scale_up, scale_down, serve_router.T)


def plain_shards(w_gate, avg_gate, w_up, avg_up, w_down, avg_down, router_weight, router_gain):
    def served(w, a, axis, split):
        fresh = w + a.astype(jnp.float32)
        scale = jnp.sqrt(lax.psum(jnp.sum(fresh * fresh, axis=axis), "rows"))
        narrow = (fresh / jnp.expand_dims(scale, axis)).astype(jnp.bfloat16)
        serve = lax.all_to_all(narrow, "rows", split_axis=split, concat_axis=axis, tiled=True)
        width = serve.shape[split]
        return serve, lax.dynamic_slice_in_dim(scale, lax.axis_index("rows") * width, width, axis=1)

    serve_gate, scale_gate = served(w_gate, avg_gate, 1, 2)
    serve_up, scale_up = served(w_up, avg_up, 1, 2)
    serve_down, scale_down = served(w_down, avg_down, 2, 1)
    part_router = (router_weight * router_gain[:, None]).astype(jnp.bfloat16)
    row_router = lax.all_gather(part_router, "rows", axis=0, tiled=True)
    serve_router = lax.all_gather(row_router, "owner", axis=1, tiled=True)
    return (serve_gate, serve_up, serve_down, scale_gate, scale_up, scale_down, serve_router)


def solution(mesh):
    parts, owners = mesh.shape["rows"], mesh.shape["owner"]

    def dispatched(*args):
        experts, high, wide = args[0].shape
        tall, deep = args[4].shape[1:]
        block, slab = wide // parts, tall // parts
        columns = args[6].shape[1]
        aligned = block == LANES and slab == LANES and deep % LANES == 0 and high % LANES == 0
        aligned = aligned and high <= 256 and deep <= 256 and experts <= 16 and experts % 8 == 0
        aligned = aligned and experts > EARLY and columns % 16 == 0 and parts == 8 and owners > 1
        return shards(parts, owners, *args) if aligned else plain_shards(*args)

    return jax.shard_map(
        dispatched,
        mesh=mesh,
        in_specs=(
            P("owner", "rows", None),
            P("owner", "rows", None),
            P("owner", "rows", None),
            P("owner", "rows", None),
            P("owner", None, "rows"),
            P("owner", None, "rows"),
            P("rows", "owner"),
            P("rows"),
        ),
        out_specs=(
            P("owner", None, "rows"),
            P("owner", None, "rows"),
            P("owner", "rows", None),
            P("owner", "rows"),
            P("owner", "rows"),
            P("owner", "rows"),
            P(),
        ),
        check_vma=False,
    )
```

```python
import functools

import jax
import jax.numpy as jnp
from jax import lax
from jax.experimental import pallas as pl
from jax.experimental.pallas import tpu as pltpu
from jax.sharding import PartitionSpec as P

LANES = 128
EARLY = 8
RING = 4
TAIL = 3
MESH = pl.DeviceIdType.MESH


def remote(src, dst, send, recv, peer, axis="rows"):
    return pltpu.make_async_remote_copy(
        src_ref=src, dst_ref=dst, send_sem=send, recv_sem=recv, device_id={axis: peer}, device_id_type=MESH
    )


def regroup(
    parts, owners,
    wg, ag, wu, au, wd, ad, rw, gain,
    og, ou, od, *refs,
):
    ot, (oscale, orouter, *refs) = refs[: parts // 2], refs[parts // 2 :]
    (
    wbuf, abuf, wdbuf, adbuf, sg, su, sd, direct, near, early, early_heard, early_factors,
    rest, rest_heard, factors, scales, rwbuf, gainbuf, router,
    in_sem, down_sem, direct_send, direct_recv, early_send, early_recv, give_send, give_recv, back_send, back_recv,
    data_send, data_recv, kept, strip_send, strip_recv, router_send, router_recv, small,
    ) = refs
    me = lax.axis_index("rows")
    own = lax.axis_index("owner")
    experts, high = wg.shape[0], wg.shape[1]
    deep = wd.shape[2]
    tail = ot[0].shape[0]
    levels = parts.bit_length() - 1
    bits = [lax.rem(me // 2**level, 2) for level in range(levels)]

    def peer(k):
        return lax.rem(me + k, parts)

    def mirrored(index):
        return sum(lax.rem(index // 2**i, 2) * 2 ** (levels - 1 - i) for i in range(levels))

    def fetch(w, a, e, wv, av, sem, slot):
        pltpu.make_async_copy(w.at[e], wv.at[slot], sem.at[0, slot]).start()
        pltpu.make_async_copy(a.at[e], av.at[slot], sem.at[1, slot]).start()

    def fetched(w, a, e, wv, av, sem, slot):
        pltpu.make_async_copy(w.at[e], wv.at[slot], sem.at[0, slot]).wait()
        pltpu.make_async_copy(a.at[e], av.at[slot], sem.at[1, slot]).wait()

    def landed(ref, sem):
        pltpu.make_async_copy(ref, ref, sem).wait()

    def stream(w, a, wv, av, sem, base, first, count, body):
        for i in range(min(RING - 1, count)):
            fetch(w, a, first + i, wv, av, sem, base + i)

        @pl.loop(0, count)
        def _(i):
            slot = base + lax.rem(i, RING)
            fetched(w, a, first + i, wv, av, sem, slot)

            @pl.when(i + RING - 1 < count)
            def _():
                fetch(w, a, first + i + RING - 1, wv, av, sem, base + lax.rem(i + RING - 1, RING))

            body(first + i, slot)

    def lanes(p):
        return pl.ds(pl.multiple_of(p * LANES, LANES), LANES)

    def columns_sum(slot, put):
        @pl.loop(0, parts)
        def _(s):
            p = mirrored(s)
            fresh = wbuf[slot, :, lanes(p)] + abuf[slot, :, lanes(p)].astype(jnp.float32)
            put(s, jnp.sum(fresh * fresh, axis=0, keepdims=True))

    def rows_sum(slot, put):
        @pl.loop(0, parts)
        def _(s):
            p = mirrored(s)
            fresh = wdbuf[slot, lanes(p), :] + adbuf[slot, lanes(p), :].astype(jnp.float32)
            square = fresh * fresh
            folded = square[:, :LANES]
            for start in range(LANES, deep, LANES):
                folded = folded + square[:, start : start + LANES]
            put(s, jnp.sum(folded.T, axis=0, keepdims=True))

    def columns_norm(take, e, slot, send, first=0, count=high):
        rows = pl.ds(first, count)

        @pl.loop(0, parts)
        def _(s):
            p = mirrored(s)
            fresh = wbuf[slot, rows, lanes(p)] + abuf[slot, rows, lanes(p)].astype(jnp.float32)
            send[e, p, rows, :] = (fresh * take(s)).astype(send.dtype)

    def rows_norm(take, e, slot):
        @pl.loop(0, parts)
        def _(s):
            p = mirrored(s)
            factor = jnp.broadcast_to(take(s), (LANES, LANES)).T
            for start in range(0, deep, LANES):
                fresh = wdbuf[slot, lanes(p), start : start + LANES]
                fresh = fresh + adbuf[slot, lanes(p), start : start + LANES].astype(jnp.float32)
                sd[e, p, :, start : start + LANES] = (fresh * factor).astype(sd.dtype)

    def put_first(s, row):
        direct[me, pl.ds(s, 1), :] = row
        early[s, 0:1, :] = row

    def put_in(ref, row):
        def put(s, value):
            ref[s, pl.ds(row, 1), :] = value

        return put

    def taken(ref, row):
        return lambda s: ref[s, pl.ds(row, 1), :]

    def push(kind, e):
        send, stage = ((sg, og), (su, ou), (sd, od))[kind]
        if kind < 2:
            place = stage.at[e, pl.ds(pl.multiple_of(me * high, high), high), :]
        else:
            place = stage.at[e, :, pl.ds(pl.multiple_of(me * deep, deep), deep)]

        @pl.loop(1, parts)
        def _(k):
            remote(send.at[e, peer(k)], place, data_send.at[kind], data_recv.at[kind], peer(k)).start()

        pltpu.make_async_copy(send.at[e, me], place, kept.at[kind]).start()

    def push_first(half):
        rows = pl.ds(half * (high // 2), high // 2)
        place = og.at[0, pl.ds(pl.multiple_of(me * high + half * (high // 2), high // 2), high // 2), :]

        @pl.loop(1, parts)
        def _(k):
            remote(sg.at[0, peer(k), rows, :], place, data_send.at[0], data_recv.at[0], peer(k)).start()

        pltpu.make_async_copy(sg.at[0, me, rows, :], place, kept.at[0]).start()

    def flipped(mask):
        return me + sum((1 - 2 * bits[i]) * 2**i for i in range(levels) if mask >> i & 1)

    def partner(level):
        return flipped(1 << level)

    def strip(block):
        return router.at[own, :, pl.ds(pl.multiple_of(block * high, high), high)]

    def strips_out(level):
        blocks = [me]
        for further in range(levels - 1, level, -1):
            blocks = blocks + [b + (1 - 2 * bits[further]) * 2**further for b in blocks]
        for block in blocks:
            remote(strip(block), strip(block), strip_send.at[level], strip_recv.at[level], partner(level)).start()

    def strips_in(level):
        landed(router.at[own, :, pl.ds(0, (parts >> (level + 1)) * high)], strip_recv.at[level])

    def span(level):
        half = parts >> (level + 1)
        start = sum(bits[i] * (parts >> (i + 1)) for i in range(level))
        return start + bits[level] * half, start + (1 - bits[level]) * half, half

    def heard(level):
        return rest_heard.at[pl.ds(parts - (parts >> level), parts >> (level + 1))]

    def give(level):
        _, away, half = span(level)
        remote(
            rest.at[pl.ds(away, half)], heard(level), give_send.at[level], give_recv.at[level], partner(level)
        ).start()

    def gain_level(level):
        keep, _, half = span(level)
        landed(heard(level), give_recv.at[level])
        first = parts - (parts >> level)
        for i in range(half):
            rest[keep + i] = rest[keep + i] + rest_heard[first + i]

    def back(level):
        keep, _, half = span(level)
        mine = factors.at[pl.ds(keep, half)]
        remote(mine, mine, back_send.at[level], back_recv.at[level], partner(level)).start()

    def regain(level):
        half = parts >> (level + 1)
        landed(factors.at[pl.ds(0, half)], back_recv.at[level])

    barrier = pltpu.get_barrier_semaphore()
    fetch(wg, ag, 0, wbuf, abuf, in_sem, 0)
    fetch(wg, ag, 1, wbuf, abuf, in_sem, 1)
    pltpu.make_async_copy(rw, rwbuf, small.at[0]).start()
    pltpu.make_async_copy(gain, gainbuf, small.at[1]).start()

    @pl.loop(1, parts)
    def _(k):
        pl.semaphore_signal(barrier, inc=1, device_id={"rows": peer(k)}, device_id_type=MESH)

    for k in range(1, owners):
        pl.semaphore_signal(barrier, inc=1, device_id={"owner": lax.rem(own + k, owners)}, device_id_type=MESH)

    fetched(wg, ag, 0, wbuf, abuf, in_sem, 0)
    for later in (2, 3):
        fetch(wg, ag, later, wbuf, abuf, in_sem, later)
    columns_sum(0, put_first)
    landed(rwbuf, small.at[0])
    landed(gainbuf, small.at[1])
    router[own, :, pl.ds(pl.multiple_of(me * high, high), high)] = (rwbuf[...] * gainbuf[...]).astype(router.dtype)
    pl.semaphore_wait(barrier, parts - 1 + owners - 1)

    @pl.loop(1, parts)
    def _(k):
        remote(direct.at[me], direct.at[me], direct_send, direct_recv, peer(k)).start()

    strips_out(levels - 1)
    for later in range(4, EARLY):
        fetch(wg, ag, later, wbuf, abuf, in_sem, later)

    @pl.loop(1, EARLY)
    def _(unit):
        fetched(wg, ag, unit, wbuf, abuf, in_sem, unit)
        columns_sum(unit, put_in(early, unit))

    landed(direct.at[pl.ds(0, parts - 1)], direct_recv)
    total = direct[0]
    for source in range(1, parts):
        total = total + direct[source]
    near[...] = 1.0 / jnp.sqrt(total)

    def first_factor(s):
        return near[pl.ds(s, 1), :]

    columns_norm(first_factor, 0, 0, sg, 0, high // 2)

    @pl.loop(1, parts)
    def _(k):
        remote(early.at[mirrored(peer(k))], early_heard.at[me], early_send.at[0], early_recv.at[0], peer(k)).start()

    push_first(0)
    columns_norm(first_factor, 0, 0, sg, high // 2, high // 2)
    landed(early_heard.at[pl.ds(0, parts - 1)], early_recv.at[0])
    mine = mirrored(me)
    total = early[mine]
    for k in range(1, parts):
        total = total + early_heard[peer(k)]
    scale = jnp.sqrt(total)
    scales[0:EARLY] = scale
    early_factors[mine] = 1.0 / scale

    @pl.loop(1, parts)
    def _(k):
        ref = early_factors.at[mine]
        remote(ref, ref, early_send.at[1], early_recv.at[1], peer(k)).start()

    push_first(1)
    first_up, first_down = experts - EARLY, 2 * experts - EARLY
    stream(
        wg, ag, wbuf, abuf, in_sem, EARLY, EARLY, experts - EARLY,
        lambda e, slot: columns_sum(slot, put_in(rest, e - EARLY)),
    )
    landed(early_factors.at[pl.ds(0, parts - 1)], early_recv.at[1])

    @pl.loop(1, 3)
    def _(unit):
        columns_norm(taken(early_factors, unit), unit, unit, sg)

    push(0, 1)

    @pl.loop(3, EARLY)
    def _(unit):
        columns_norm(taken(early_factors, unit), unit, unit, sg)

    push(0, 2)
    for level in range(levels - 1, 1, -1):
        strips_in(level)
        strips_out(level - 1)
    stream(
        wu, au, wbuf, abuf, in_sem, EARLY, 0, experts,
        lambda e, slot: columns_sum(slot, put_in(rest, first_up + e)),
    )
    push(0, 3)
    stream(
        wd, ad, wdbuf, adbuf, down_sem, 0, 0, experts,
        lambda e, slot: rows_sum(slot, put_in(rest, first_down + e)),
    )
    strips_in(1)
    strips_out(0)
    give(0)
    gain_level(0)
    sent = 4
    for level in range(1, levels):
        give(level)
        push(0, sent)
        sent += 1
        gain_level(level)
    keep = span(levels - 1)[0]
    scale = jnp.sqrt(rest[keep])
    scales[EARLY:] = scale
    factors[keep] = 1.0 / scale
    pltpu.make_async_copy(scales, oscale, small.at[0]).start()
    for level in range(levels - 1, 0, -1):
        back(level)
        push(0, sent)
        sent += 1
        regain(level)
    for left in range(sent, EARLY):
        push(0, left)
    back(0)
    regain(0)

    def gate(e, slot):
        columns_norm(taken(factors, e - EARLY), e, slot, sg)

        @pl.when(e > EARLY)
        def _():
            push(0, e - 1)

    def up(e, slot):
        columns_norm(taken(factors, first_up + e), e, slot, su)

        @pl.when(e > 0)
        def _():
            push(1, e - 1)

    def down(e, slot):
        rows_norm(taken(factors, first_down + e), e, slot)

        @pl.when(e > 0)
        def _():
            push(2, e - 1)

    stream(wg, ag, wbuf, abuf, in_sem, EARLY, EARLY, experts - EARLY, gate)
    push(0, experts - 1)

    stream(
        wd, ad, wdbuf, adbuf, down_sem, 0, experts - tail, tail,
        lambda e, slot: rows_norm(taken(factors, first_down + e), e, slot),
    )
    strips_in(0)
    for mask in range(parts // 2):
        far = sd.at[pl.ds(experts - tail, tail), flipped(parts // 2 + mask)]
        pltpu.make_async_copy(far, ot[mask], kept.at[3]).start()
    place = od.at[pl.ds(experts - tail, tail), :, pl.ds(pl.multiple_of(me * deep, deep), deep)]
    for mask in range(1, parts // 2):
        there = flipped(mask)
        remote(
            sd.at[pl.ds(experts - tail, tail), there], place, data_send.at[3], data_recv.at[3], there
        ).start()
    pltpu.make_async_copy(sd.at[pl.ds(experts - tail, tail), me], place, kept.at[4]).start()
    for k in range(1, owners):
        remote(
            router.at[own], router.at[own], router_send, router_recv, lax.rem(own + k, owners), "owner"
        ).start()

    stream(wu, au, wbuf, abuf, in_sem, EARLY, 0, experts, up)
    push(1, experts - 1)
    stream(wd, ad, wdbuf, adbuf, down_sem, 0, 0, experts - tail, down)
    push(2, experts - tail - 1)


    arrived = router.at[pl.ds(0, owners - 1)]
    landed(arrived, router_recv)
    pltpu.make_async_copy(router, orouter, small.at[1]).start()

    landed(direct.at[pl.ds(0, parts - 1)], direct_send)
    landed(early.at[pl.ds(0, parts - 1)], early_send.at[0])
    landed(early.at[pl.ds(0, parts - 1)], early_send.at[1])
    for level in range(levels):
        half = rest.at[pl.ds(0, parts >> (level + 1))]
        landed(half, give_send.at[level])
        landed(half, back_send.at[level])
        landed(router.at[own, :, pl.ds(0, (parts >> (level + 1)) * high)], strip_send.at[level])
    landed(arrived, router_send)
    pltpu.make_async_copy(scales, oscale, small.at[0]).wait()
    pltpu.make_async_copy(router, orouter, small.at[1]).wait()
    halves = sd.at[pl.ds(experts - tail, tail), pl.ds(0, parts // 2)]
    nearer = sd.at[pl.ds(experts - tail, tail), pl.ds(0, parts // 2 - 1)]
    landed(halves, kept.at[3])
    landed(sd.at[pl.ds(experts - tail, tail), 0], kept.at[4])
    landed(nearer, data_send.at[3])
    landed(nearer, data_recv.at[3])
    for kind, send in enumerate((sg, su, sd)):
        count = experts - tail if kind == 2 else experts
        landed(send.at[pl.ds(0, count), 0], kept.at[kind])
        most = send.at[pl.ds(0, count), pl.ds(0, parts - 1)]
        landed(most, data_send.at[kind])
        landed(most, data_recv.at[kind])


def publish(depth, sg, su, sd, scale, router, og, ou, od, o1, o2, o3, orouter, tall, flat, sbuf, rbuf, load, store, small):
    slots = tall.shape[0]
    experts = og.shape[0]
    jobs = [(stage, out, tall, e) for stage, out in ((sg, og), (su, ou)) for e in range(experts)]
    jobs += [(sd, od, flat, e) for e in range(experts)]

    def read(i):
        stage, _, buffer, e = jobs[i]
        return pltpu.make_async_copy(stage.at[e], buffer.at[i % slots], load.at[i % slots])

    def write(i):
        _, out, buffer, e = jobs[i]
        return pltpu.make_async_copy(buffer.at[i % slots], out.at[e], store.at[i % slots])

    extras = [pltpu.make_async_copy(scale, sbuf, small.at[0]), pltpu.make_async_copy(router, rbuf, small.at[1])]
    for copy in extras:
        copy.start()
    for i in range(len(jobs) + depth):
        if i < len(jobs):
            if i >= slots:
                write(i - slots).wait()
            read(i).start()
        if i >= depth:
            read(i - depth).wait()
            write(i - depth).start()
    for copy in extras:
        copy.wait()
    outs = [pltpu.make_async_copy(sbuf.at[pl.ds(i * experts, experts)], o, small.at[2 + i]) for i, o in enumerate((o1, o2, o3))]
    columns = rbuf.shape[1]
    for i in range(rbuf.shape[0]):
        outs.append(pltpu.make_async_copy(rbuf.at[i], orouter.at[pl.ds(i * columns, columns)], small.at[5 + i]))
    for copy in outs:
        copy.start()
    for i in range(max(0, len(jobs) - slots), len(jobs)):
        write(i).wait()
    for copy in outs:
        copy.wait()


def stack_columns(parts, *refs):
    *xs, _, o, sem = refs
    me, half = lax.axis_index("rows"), len(xs)
    tail, _, deep = xs[0].shape
    copies = []
    for mask, x in enumerate(xs):
        levels = parts.bit_length() - 1
        source = sum(lax.rem(me // 2**i + (half + mask >> i & 1), 2) * 2**i for i in range(levels))
        place = o.at[pl.ds(o.shape[0] - tail, tail), :, pl.ds(pl.multiple_of(source * deep, deep), deep)]
        copies.append(pltpu.make_async_copy(x, place, sem.at[mask]))
    for copy in copies:
        copy.start()
    for copy in copies:
        copy.wait()


def shards(parts, owners, w_gate, avg_gate, w_up, avg_up, w_down, avg_down, router_weight, router_gain):
    experts, high, wide = w_gate.shape
    tall, deep = w_down.shape[1:]
    block, slab = wide // parts, tall // parts
    units, slots, later = 3 * experts, EARLY + RING, 3 * experts - EARLY
    columns, model = router_weight.shape[1], parts * high
    levels = parts.bit_length() - 1
    f32, bf16 = jnp.float32, jnp.bfloat16
    any_spec = pl.BlockSpec(memory_space=pl.ANY)
    shape_columns, shape_down = (experts, high * parts, block), (experts, slab, deep * parts)
    dma = pltpu.SemaphoreType.DMA

    *stages, scales, routers = pl.pallas_call(
        functools.partial(regroup, parts, owners),
        in_specs=[any_spec] * 8,
        out_specs=[any_spec] * (5 + parts // 2),
        out_shape=[
            jax.ShapeDtypeStruct(shape_columns, bf16),
            jax.ShapeDtypeStruct(shape_columns, bf16),
            jax.ShapeDtypeStruct(shape_down, bf16),
            *[jax.ShapeDtypeStruct((TAIL, slab, deep), bf16)] * (parts // 2),
            jax.ShapeDtypeStruct((units, LANES), f32),
            jax.ShapeDtypeStruct((owners, columns, model), bf16),
        ],
        scratch_shapes=[
            pltpu.VMEM((slots, high, wide), f32),
            pltpu.VMEM((slots, high, wide), bf16),
            pltpu.VMEM((RING, tall, deep), f32),
            pltpu.VMEM((RING, tall, deep), bf16),
            pltpu.VMEM((experts, parts, high, block), bf16),
            pltpu.VMEM((experts, parts, high, block), bf16),
            pltpu.VMEM((experts, parts, slab, deep), bf16),
            pltpu.VMEM((parts, parts, LANES), f32),
            pltpu.VMEM((parts, LANES), f32),
            pltpu.VMEM((parts, EARLY, LANES), f32),
            pltpu.VMEM((parts, EARLY, LANES), f32),
            pltpu.VMEM((parts, EARLY, LANES), f32),
            pltpu.VMEM((parts, later, LANES), f32),
            pltpu.VMEM((parts - 1, later, LANES), f32),
            pltpu.VMEM((parts, later, LANES), f32),
            pltpu.VMEM((units, LANES), f32),
            pltpu.VMEM((columns, high), f32),
            pltpu.VMEM((1, high), f32),
            pltpu.VMEM((owners, columns, model), bf16),
            dma((2, slots)), dma((2, RING)), dma, dma, dma((2,)), dma((2,)),
            dma((levels,)), dma((levels,)), dma((levels,)), dma((levels,)),
            dma((4,)), dma((4,)), dma((5,)), dma((levels,)), dma((levels,)), dma, dma, dma((2,)),
        ],
        cost_estimate=pl.CostEstimate(flops=2**30, bytes_accessed=2**28, transcendentals=0),
        compiler_params=pltpu.CompilerParams(
            collective_id=0, has_side_effects=True, vmem_limit_bytes=60 * 2**20
        ),
    )(w_gate, avg_gate, w_up, avg_up, w_down, avg_down, router_weight.T, router_gain.reshape(1, high))

    stages, pieces = stages[:3], stages[3:]
    got = [
        lax.ppermute(x, "rows", [(i, i ^ (parts // 2 + mask)) for i in range(parts)])
        for mask, x in enumerate(pieces)
    ]
    serve_gate, serve_up, held, scale_gate, scale_up, scale_down, serve_router = pl.pallas_call(
        functools.partial(publish, 8),
        in_specs=[any_spec] * 5,
        out_specs=[any_spec] * 7,
        out_shape=[
            jax.ShapeDtypeStruct(shape_columns, bf16),
            jax.ShapeDtypeStruct(shape_columns, bf16),
            jax.ShapeDtypeStruct(shape_down, bf16),
            *[jax.ShapeDtypeStruct((experts, LANES), f32)] * 3,
            jax.ShapeDtypeStruct((owners * columns, model), bf16),
        ],
        scratch_shapes=[
            pltpu.VMEM((16,) + shape_columns[1:], bf16),
            pltpu.VMEM((16,) + shape_down[1:], bf16),
            pltpu.VMEM((units, LANES), f32),
            pltpu.VMEM((owners, columns, model), bf16),
            dma((16,)), dma((16,)), dma((5 + owners,)),
        ],
        cost_estimate=pl.CostEstimate(flops=2**26, bytes_accessed=2**26, transcendentals=0),
        compiler_params=pltpu.CompilerParams(vmem_limit_bytes=62 * 2**20),
    )(*stages, scales, routers)
    serve_down = pl.pallas_call(
        functools.partial(stack_columns, parts),
        in_specs=[pl.BlockSpec(memory_space=pltpu.VMEM)] * len(got) + [any_spec],
        out_specs=any_spec,
        out_shape=jax.ShapeDtypeStruct(shape_down, bf16),
        scratch_shapes=[dma((len(got),))],
        input_output_aliases={len(got): 0},
        cost_estimate=pl.CostEstimate(flops=2**21, bytes_accessed=2**22, transcendentals=0),
        compiler_params=pltpu.CompilerParams(vmem_limit_bytes=16 * 2**20),
    )(*got, held)
    return (serve_gate, serve_up, serve_down, scale_gate, scale_up, scale_down, serve_router.T)


def plain_shards(w_gate, avg_gate, w_up, avg_up, w_down, avg_down, router_weight, router_gain):
    def served(w, a, axis, split):
        fresh = w + a.astype(jnp.float32)
        scale = jnp.sqrt(lax.psum(jnp.sum(fresh * fresh, axis=axis), "rows"))
        narrow = (fresh / jnp.expand_dims(scale, axis)).astype(jnp.bfloat16)
        serve = lax.all_to_all(narrow, "rows", split_axis=split, concat_axis=axis, tiled=True)
        width = serve.shape[split]
        return serve, lax.dynamic_slice_in_dim(scale, lax.axis_index("rows") * width, width, axis=1)

    serve_gate, scale_gate = served(w_gate, avg_gate, 1, 2)
    serve_up, scale_up = served(w_up, avg_up, 1, 2)
    serve_down, scale_down = served(w_down, avg_down, 2, 1)
    part_router = (router_weight * router_gain[:, None]).astype(jnp.bfloat16)
    row_router = lax.all_gather(part_router, "rows", axis=0, tiled=True)
    serve_router = lax.all_gather(row_router, "owner", axis=1, tiled=True)
    return (serve_gate, serve_up, serve_down, scale_gate, scale_up, scale_down, serve_router)


def solution(mesh):
    parts, owners = mesh.shape["rows"], mesh.shape["owner"]

    def dispatched(*args):
        experts, high, wide = args[0].shape
        tall, deep = args[4].shape[1:]
        block, slab = wide // parts, tall // parts
        columns = args[6].shape[1]
        aligned = block == LANES and slab == LANES and deep % LANES == 0 and high % LANES == 0
        aligned = aligned and high <= 256 and deep <= 256 and experts <= 16 and experts % 8 == 0
        aligned = aligned and experts > EARLY and columns % 16 == 0 and parts == 8 and owners > 1
        return shards(parts, owners, *args) if aligned else plain_shards(*args)

    return jax.shard_map(
        dispatched,
        mesh=mesh,
        in_specs=(
            P("owner", "rows", None),
            P("owner", "rows", None),
            P("owner", "rows", None),
            P("owner", "rows", None),
            P("owner", None, "rows"),
            P("owner", None, "rows"),
            P("rows", "owner"),
            P("rows"),
        ),
        out_specs=(
            P("owner", None, "rows"),
            P("owner", None, "rows"),
            P("owner", "rows", None),
            P("owner", "rows"),
            P("owner", "rows"),
            P("owner", "rows"),
            P(),
        ),
        check_vma=False,
    )
```
